32 devices in a mesh: gx: 4 (over z), gy: 2 (over y), ea: 4 (over x, core).
Axes of the slice: x: 2, y: 2, z: 4, core: 2. Of those that a mesh axis runs over, the one named last changes fastest.
Arguments:
- load_displacement: float32 [3, 16, 32, 512], P(None, 'gx', 'gy', 'ea'), may hold values from -6 to 6
- load_enriched: float32 [15, 8192], P(None, ('gx', 'gy', 'ea')), may hold values from -24 to 24
- stiffness_shift: float32 [16, 32, 512], P('gx', 'gy', 'ea'), may hold values from 2 to 8
- enriched_diag: float32 [15, 8192], P(None, ('gx', 'gy', 'ea')), may hold values from 11 to 17
- enriched_off: float32 [15, 15, 8192], P(None, None, ('gx', 'gy', 'ea')), may hold values from -0.4 to 0.4
- coupling: float32 [3, 15, 16384], P(None, None, ('gx', 'gy', 'ea')), may hold values from -0.15 to 0.15
- slot_kind: int32 [32, 4, 128], P(('gx', 'gy', 'ea')), may hold values from 0 to 2, as said below
- slot_cell: int32 [32, 4, 128], P(('gx', 'gy', 'ea')), may hold values from 0 to 8191, as said below
- slot_node: int32 [32, 4, 128], P(('gx', 'gy', 'ea')), may hold values from 0 to 255, as said below
Outputs:
- solution_displacement: float32 [3, 16, 32, 512], P(None, 'gx', 'gy', 'ea')
- residual_displacement: float32 [3, 16, 32, 512], P(None, 'gx', 'gy', 'ea')
- solution_enriched: float32 [15, 8192], P(None, ('gx', 'gy', 'ea'))
- residual_enriched: float32 [15, 8192], P(None, ('gx', 'gy', 'ea'))
The draws below stay inside these ranges and needn't reach their ends.
Inputs may be any that keep to these rules, and one draw needn't show every extreme that they name: `slot_kind`: within each block of 128 slots of one device to one owner the slots of kind 1 or 2 come first; in every draw some owner receives 128 such slots from each of the 4 devices of its column. `slot_cell`: distinct within one device. `slot_node`: distinct within each block of 128 slots of one device to one owner.
All inputs are finite; a program needn't handle non-finite values.
Results may differ from the reference program's by a relative error of at most 0.0003.
Values sent between devices are 32-bit elements; how exact they have to be, the bound alone decides.
No kernel may reach another device: no remote copies, remote signals or barrier semaphores. Data moves between devices by JAX's collectives and lax.ppermute only.
A program may use at most 64 MiB of HBM per device.

```python
import jax
import jax.numpy as jnp
from jax import lax

CX = 4
CY = 16
CZ = 128
ENB = 256
CAP = 128
ECOMP = 15
ITERS = 3
NX = 16
NY = 32
NZ = 512
NE = 8192
SLOTS = 16384
N_GX = 4
N_GY = 2
N_EA = 4
DEVICES = 32


def draw_slot_cell(key, part):
    device_keys = jax.random.split(jax.random.fold_in(key, 11), DEVICES)

    def one_device(device_key):
        return jax.random.permutation(device_key, CX * CY * CZ)[:N_EA * CAP].astype(jnp.int32)
    return jax.vmap(one_device)(device_keys).reshape(DEVICES, N_EA, CAP)


def draw_slot_node(key, part):
    block_keys = jax.random.split(jax.random.fold_in(key, 17), DEVICES * N_EA)

    def one_block(block_key):
        return jax.random.permutation(block_key, ENB)[:CAP].astype(jnp.int32)
    return jax.vmap(one_block)(block_keys).reshape(DEVICES, N_EA, CAP)


def draw_slot_kind(key, part):
    live_key, kind_key, column_key, owner_key = jax.random.split(jax.random.fold_in(key, 29), 4)
    live_count = jax.random.randint(live_key, (DEVICES, N_EA), CAP // 8, CAP + 1)
    columns = DEVICES // N_EA
    column = jax.random.randint(column_key, (), 0, columns)
    target = jax.random.randint(owner_key, (), 0, N_EA)
    device_ids = jnp.arange(DEVICES, dtype=jnp.int32)[:, None]
    owner_ids = jnp.arange(N_EA, dtype=jnp.int32)[None, :]
    full_block = (device_ids // N_EA == column) & (owner_ids == target)
    live_count = jnp.where(full_block, CAP, live_count)
    slot_kinds = jax.random.randint(kind_key, (DEVICES, N_EA, CAP), 1, 3)
    position = jnp.arange(CAP, dtype=jnp.int32)[None, None, :]
    return jnp.where(position < live_count[:, :, None], slot_kinds, 0).astype(jnp.int32)


def shard_levels(own_key, extent, cuts, low, largest):
    gain, own = 1.0, jax.random.fold_in(own_key, 6)
    for dim, blocks in cuts:
        steps = jnp.exp(jax.random.uniform(jax.random.fold_in(own, dim), (blocks,), jnp.float32, low / len(cuts), largest / len(cuts)))
        gain = gain * jnp.repeat(steps, extent[dim] // blocks).reshape([-1 if axis == dim else 1 for axis in range(len(extent))])
    return gain


def gaussian(own_key, extent, spread, limit, cuts=(), kind=jnp.bfloat16):
    loudness = shard_levels(own_key, extent, cuts, -0.22, 0.18) if cuts else 1.0
    entries = jax.random.normal(own_key, extent, jnp.float32) * spread * loudness
    return jnp.minimum(jnp.maximum(entries, -limit), limit).astype(kind)


def setup_inputs(seed: int = 0) -> dict:
    seeds = jax.random.split(jax.random.key(seed), 10)
    load_displacement = gaussian(seeds[0], (3, NX, NY, NZ), 1.0, 6.0, ((1, 4), (2, 2), (3, 4)), jnp.float32)
    load_enriched = gaussian(seeds[1], (ECOMP, NE), 4.0, 24.0, ((1, 32),), jnp.float32)
    stiffness_shift = jnp.clip(2.0 + 6.0 * jax.random.uniform(seeds[2], (NX, NY, NZ), jnp.float32) ** shard_levels(seeds[2], (NX, NY, NZ), ((0, 4), (1, 2), (2, 4)), -0.2, 0.2), 2.0, 8.0)
    enriched_diag = jnp.clip(11.0 + 6.0 * jax.random.uniform(seeds[3], (ECOMP, NE), jnp.float32) ** shard_levels(seeds[3], (ECOMP, NE), ((1, 32),), -0.2, 0.2), 11.0, 17.0)
    enriched_off = jnp.clip(jax.random.uniform(seeds[4], (ECOMP, ECOMP, NE), jnp.float32, -0.4, 0.4) * shard_levels(seeds[4], (ECOMP, ECOMP, NE), ((2, 32),), -0.4, 0.0), -0.4, 0.4)
    coupling = jnp.clip(jax.random.uniform(seeds[5], (3, ECOMP, SLOTS), jnp.float32, -0.15, 0.15) * shard_levels(seeds[5], (3, ECOMP, SLOTS), ((2, 32),), -0.4, 0.0), -0.15, 0.15)
    slot_kind = draw_slot_kind(jax.random.fold_in(seeds[9], 71), 0)
    slot_cell = draw_slot_cell(jax.random.fold_in(seeds[9], 71), 0)
    slot_node = draw_slot_node(jax.random.fold_in(seeds[9], 71), 0)
    return {"load_displacement": load_displacement, "load_enriched": load_enriched, "stiffness_shift": stiffness_shift, "enriched_diag": enriched_diag, "enriched_off": enriched_off, "coupling": coupling, "slot_kind": slot_kind, "slot_cell": slot_cell, "slot_node": slot_node}


HIGHEST_PRECISION = lax.Precision.HIGHEST


def stencil(displacement, stiffness_shift):
    padded = jnp.pad(displacement, ((0, 0), (1, 1), (1, 1), (1, 1)))
    beside = padded[:, 2:, 1:-1, 1:-1] + padded[:, :-2, 1:-1, 1:-1]
    beside = beside + padded[:, 1:-1, 2:, 1:-1] + padded[:, 1:-1, :-2, 1:-1]
    beside = beside + padded[:, 1:-1, 1:-1, 2:] + padded[:, 1:-1, 1:-1, :-2]
    return (6.0 + stiffness_shift)[None] * displacement - beside


def enriched_block(enriched_diag, enriched_off):
    components = enriched_diag.shape[0]
    identity = jnp.eye(components, dtype=jnp.float32)
    symmetric = 0.5 * (enriched_off + jnp.transpose(enriched_off, (1, 0, 2)))
    return symmetric * (1.0 - identity)[:, :, None] + identity[:, :, None] * enriched_diag[:, None, :]


def slot_columns(kinds_flat):
    heaviside = (kinds_flat >= 1).astype(jnp.float32)
    tip_mask = (kinds_flat == 2).astype(jnp.float32)
    return jnp.concatenate([jnp.broadcast_to(heaviside, (3, heaviside.shape[0])), jnp.broadcast_to(tip_mask, (12, tip_mask.shape[0]))], axis=0)


def inner(first, second):
    return jnp.sum(first[0] * second[0]) + jnp.sum(first[1] * second[1])


def reference(load_displacement, load_enriched, stiffness_shift, enriched_diag, enriched_off, coupling, slot_kind, slot_cell, slot_node):
    device_ids = jnp.arange(N_GX * N_GY * N_EA, dtype=jnp.int32)[:, None, None]
    owners = jnp.arange(N_EA, dtype=jnp.int32)[None, :, None]
    column_i = device_ids // (N_GY * N_EA)
    column_j = (device_ids // N_EA) % N_GY
    layer_k = device_ids % N_EA
    cell_x = slot_cell // (CY * CZ)
    cell_y = (slot_cell // CZ) % CY
    cell_z = slot_cell % CZ
    global_cell = (((column_i * CX + cell_x) * NY + column_j * CY + cell_y) * NZ + layer_k * CZ + cell_z).reshape(-1).astype(jnp.int32)
    global_node = ((device_ids - layer_k + owners) * ENB + slot_node).reshape(-1).astype(jnp.int32)
    slot_weights = coupling * slot_columns(slot_kind.reshape(-1))[None]
    enriched_stiff = enriched_block(enriched_diag, enriched_off)
    cell_total = NX * NY * NZ

    def operate(direction):
        displacement, enriched = direction
        flat = displacement.reshape(3, cell_total)
        picked = flat[:, global_cell]
        to_nodes = jnp.einsum('ijs,is->js', slot_weights, picked, precision=HIGHEST_PRECISION)
        pushed_enriched = jnp.einsum('ijn,jn->in', enriched_stiff, enriched, precision=HIGHEST_PRECISION)
        pushed_enriched = pushed_enriched + jnp.zeros(enriched.shape, jnp.float32).at[:, global_node].add(to_nodes)
        values = enriched[:, global_node]
        to_cells = jnp.einsum('ijs,js->is', slot_weights, values, precision=HIGHEST_PRECISION)
        added = jnp.zeros((3, cell_total), jnp.float32).at[:, global_cell].add(to_cells)
        pushed_displacement = stencil(displacement, stiffness_shift) + added.reshape(displacement.shape)
        return (pushed_displacement, pushed_enriched)

    solution = (jnp.zeros_like(load_displacement), jnp.zeros_like(load_enriched))
    residual = (load_displacement, load_enriched)
    direction = residual
    norm_now = inner(residual, residual)
    for iteration in range(ITERS):
        image = operate(direction)
        alpha = norm_now / inner(direction, image)
        solution = jax.tree.map(lambda member, partner: member + alpha * partner, solution, direction)
        residual = jax.tree.map(lambda member, partner: member - alpha * partner, residual, image)
        norm_next = inner(residual, residual)
        ratio = norm_next / norm_now
        direction = jax.tree.map(lambda member, partner: member + ratio * partner, residual, direction)
        norm_now = norm_next
    return solution[0], residual[0], solution[1], residual[1]
```

```python
import functools

import jax
import jax.numpy as jnp
from jax import lax
from jax.experimental import pallas as pl
from jax.experimental.pallas import tpu as pltpu
from jax.sharding import PartitionSpec as P

ITERS = 3
CENTRE = 11.0
SPREAD = 8.0
AXES = ("gx", "gy", "ea")
F32 = jnp.float32
BF16 = jnp.bfloat16


def swap_pairs(count, first):
    pairs = []
    for i in range(first, count - 1, 2):
        pairs += [(i, i + 1), (i + 1, i)]
    return pairs


def partner(me, step, count):
    return me ^ step if count & (count - 1) == 0 else lax.rem(me + step, count)


def slot_of(me, owner, count):
    return me ^ owner if count & (count - 1) == 0 else lax.rem(me - owner + count, count)


def partner_pairs(step, count):
    if count & (count - 1) == 0:
        return [(i, i ^ step) for i in range(count)]
    return [(i, (i + step) % count) for i in range(count)]


def halves(value):
    high = value.astype(BF16)
    low = (value - high.astype(F32)).astype(BF16)
    return high, low


def iota(shape, dim):
    return lax.broadcasted_iota(jnp.int32, shape, dim)


def one_hot(flag):
    return jnp.where(flag, 1.0, 0.0).astype(BF16)


def dot(left, right, dims):
    return lax.dot_general(left, right, (dims, ((), ())), preferred_element_type=F32)


NN = ((1,), (0,))
NT = ((1,), (1,))
TN = ((0,), (0,))


class Slots:
    def __init__(self, sizes, kind_ref, cell_ref, node_ref, coupling_ref):
        owners, capacity = kind_ref.shape[1:]
        self.owners, self.capacity = owners, capacity
        total = owners * capacity
        rows, depth_z = sizes["rows"], sizes["depth_z"]
        cells = jnp.concatenate([cell_ref[0, o : o + 1, :] for o in range(owners)], axis=1)
        kinds = jnp.concatenate([kind_ref[0, o : o + 1, :] for o in range(owners)], axis=1)
        cell_row = cells // depth_z
        cell_z = cells - cell_row * depth_z
        self.row_hot = jnp.where(iota((rows, total), 0) == cell_row, 1.0, 0.0)
        self.z_hot = one_hot(iota((depth_z, total), 0) == cell_z)
        nodes = sizes["nodes"]
        self.node_hot = [
            one_hot(iota((nodes, capacity), 0) == node_ref[0, o : o + 1, :]) for o in range(owners)
        ]
        heaviside = jnp.where(kinds >= 1, 1.0, 0.0)
        tip = jnp.where(kinds == 2, 1.0, 0.0)
        enriched = sizes["enriched"]
        masks = jnp.where(iota((enriched, total), 0) < 3, heaviside, tip)
        self.weights = [coupling_ref[p] * masks for p in range(sizes["components"])]


def pack(sizes, slots, me_ea, parity, disp, enriched, outs, part_ref):
    comps, dx, dy, dz, rows, ne, nodes = (
        sizes[k] for k in ("components", "depth_x", "depth_y", "depth_z", "rows", "enriched", "nodes")
    )
    total = slots.owners * slots.capacity
    high, low = halves(disp)
    columns = dot(jnp.concatenate([high, low], axis=0), slots.z_hot, NN)
    columns = columns[: comps * rows] + columns[comps * rows :]
    to_nodes = jnp.zeros((ne, total), F32)
    for p in range(comps):
        picked = jnp.sum(slots.row_hot * columns[p * rows : (p + 1) * rows], axis=0, keepdims=True)
        to_nodes = to_nodes + slots.weights[p] * picked
    node_high, node_low = halves(to_nodes)
    for o in range(slots.owners):
        block = slice(o * slots.capacity, (o + 1) * slots.capacity)
        part_ref[o] = dot(node_high[:, block], slots.node_hot[o], NT) + dot(
            node_low[:, block], slots.node_hot[o], NT
        )
    edge = one_hot(
        (iota((8, dz), 0) == 0) & (iota((8, dz), 1) == 0)
        | (iota((8, dz), 0) == 1) & (iota((8, dz), 1) == dz - 1)
    )
    faces = dot(edge, high, NT) + dot(edge, low, NT)
    for k, out in enumerate(outs["ea"]):
        out[:ne] = enriched
        out[ne + 1 : 2 * ne + 1] = part_ref[partner(me_ea, k + 1, slots.owners)]
        out[ne : ne + 1, : comps * rows] = faces[0:1]
        out[2 * ne + 1 : 2 * ne + 2, : comps * rows] = faces[1:2]
    grid = disp.reshape(comps, dx, dy, dz)
    even_x, even_y = parity
    first_x, last_x = grid[:, 0], grid[:, dx - 1]
    for j, out in enumerate(outs["gx"]):
        out[...] = jnp.where(even_x == (j == 0), last_x, first_x)
    lines = disp.reshape(comps * dx, dy, dz)
    for j, out in enumerate(outs["gy"]):
        out[...] = jnp.where(even_y == (j == 0), lines[:, dy - 1], lines[:, 0])


def apply(sizes, slots, me_ea, parity, disp, enriched, shift, stiff, got, own_part, held_ref):
    comps, dx, dy, dz, rows, ne, nodes = (
        sizes[k] for k in ("components", "depth_x", "depth_y", "depth_z", "rows", "enriched", "nodes")
    )
    diag_ref, off_ref = stiff
    owners = slots.owners
    wide = held_ref.shape[2]
    held_ref[0, :ne] = enriched
    for k, ref in enumerate(got["ea"]):
        held_ref[k + 1] = ref[...]
    values = []
    for o in range(owners):
        w_high, w_low = halves(held_ref[slot_of(me_ea, o, owners), :ne, :])
        values.append(dot(w_high, slots.node_hot[o], NN) + dot(w_low, slots.node_hot[o], NN))
    values = jnp.concatenate(values, axis=1)
    spread_high, spread_low = [], []
    for p in range(comps):
        to_cells = jnp.sum(slots.weights[p] * values, axis=0, keepdims=True)
        c_high, c_low = halves(to_cells)
        spread_high.append((slots.row_hot * c_high.astype(F32)).astype(BF16))
        spread_low.append((slots.row_hot * c_low.astype(F32)).astype(BF16))
    added = dot(jnp.concatenate(spread_high + spread_low, axis=0), slots.z_hot, NT)
    added = added[: comps * rows] + added[comps * rows :]
    even_x, even_y = parity
    zero_x = jnp.zeros((comps, dy, dz), F32)
    zero_y = jnp.zeros((comps * dx, dz), F32)
    x_a = got["gx"][0][...] if len(got["gx"]) > 0 else zero_x
    x_b = got["gx"][1][...] if len(got["gx"]) > 1 else zero_x
    y_a = got["gy"][0][...] if len(got["gy"]) > 0 else zero_y
    y_b = got["gy"][1][...] if len(got["gy"]) > 1 else zero_y
    below_x = jnp.where(even_x, x_b, x_a)
    above_x = jnp.where(even_x, x_a, x_b)
    below_y = jnp.where(even_y, y_b, y_a)
    above_y = jnp.where(even_y, y_a, y_b)
    grid = disp.reshape(comps, dx, dy, dz)
    beside = jnp.concatenate([grid[:, 1:], above_x[:, None]], axis=1)
    beside = beside + jnp.concatenate([below_x[:, None], grid[:, :-1]], axis=1)
    beside = beside.reshape(comps * rows, dz)
    total_rows = comps * rows
    y_place = iota((total_rows, dz), 0) % dy
    spread_y = (comps * dx, dy, dz)
    low_y = jnp.broadcast_to(below_y[:, None, :], spread_y).reshape(total_rows, dz)
    high_y = jnp.broadcast_to(above_y[:, None, :], spread_y).reshape(total_rows, dz)
    beside = beside + jnp.where(y_place == 0, low_y, pltpu.roll(disp, 1, 0))
    beside = beside + jnp.where(y_place == dy - 1, high_y, pltpu.roll(disp, total_rows - 1, 0))
    z_place = iota((total_rows, dz), 1)
    beside = beside + jnp.where(z_place == 0, 0.0, pltpu.roll(disp, 1, 1))
    beside = beside + jnp.where(z_place == dz - 1, 0.0, pltpu.roll(disp, dz - 1, 1))
    below = jnp.maximum(me_ea - 1, 0)
    above = jnp.minimum(me_ea + 1, owners - 1)
    low_z = held_ref[slot_of(me_ea, below, owners), 2 * ne + 1 : 2 * ne + 2, :total_rows]
    high_z = held_ref[slot_of(me_ea, above, owners), ne : ne + 1, :total_rows]
    low_z = jnp.where(me_ea > 0, low_z, 0.0)
    high_z = jnp.where(me_ea < owners - 1, high_z, 0.0)
    line = iota((8, total_rows), 0)
    lows, highs = halves(low_z), halves(high_z)
    sides = jnp.zeros((8, total_rows), F32)
    for j, part in enumerate((lows[0], lows[1], highs[0], highs[1])):
        sides = jnp.where(line == j, part.astype(F32), sides)
    edge_row, edge_lane = iota((8, dz), 0), iota((8, dz), 1)
    edge = one_hot((edge_row < 2) & (edge_lane == 0) | (edge_row >= 2) & (edge_row < 4) & (edge_lane == dz - 1))
    beside = beside + dot(sides.astype(BF16), edge, TN)
    scale = (6.0 - CENTRE) + shift
    scaled = (scale[None] * disp.reshape(comps, rows, dz)).reshape(total_rows, dz)
    next_disp = (scaled - beside + added) * (1.0 / SPREAD)
    node_terms = own_part
    for ref in got["ea"]:
        node_terms = node_terms + ref[ne + 1 : 2 * ne + 1]
    row = iota((ne, nodes), 0)
    across = jnp.zeros((ne, nodes), F32)
    along = jnp.zeros((ne, nodes), F32)
    for q in range(ne):
        off = jnp.where(row == q, 0.0, off_ref[q])
        across = across + off * enriched[q : q + 1]
        along = jnp.where(row == q, jnp.sum(off * enriched, axis=0, keepdims=True), along)
    pushed = 0.5 * (across + along) + (diag_ref[...] - CENTRE) * enriched
    next_enriched = (pushed + node_terms) * (1.0 / SPREAD)
    return next_disp, next_enriched


def partial_product(first, second):
    grid = first[0] * second[0]
    total = jnp.sum(grid, axis=0, keepdims=True)
    nodes = jnp.sum(first[1] * second[1], axis=0, keepdims=True)
    lanes = grid.shape[1]
    for j in range(nodes.shape[1] // lanes):
        total = total + nodes[:, j * lanes : (j + 1) * lanes]
    return total


def places(sizes):
    return lax.axis_index("ea"), (lax.axis_index("gx") % 2 == 0, lax.axis_index("gy") % 2 == 0)


def split_outs(sizes, refs):
    n_x, n_y, n_e = sizes["x_swaps"], sizes["y_swaps"], sizes["others"]
    return {"gx": refs[:n_x], "gy": refs[n_x : n_x + n_y], "ea": refs[n_x + n_y : n_x + n_y + n_e]}


def first_kernel(sizes, *refs):
    disp_ref, enr_ref, kind_ref, cell_ref, node_ref, coupling_ref = refs[:6]
    n = sizes["messages"]
    outs = split_outs(sizes, refs[6 : 6 + n])
    own_ref, part_ref = refs[6 + n], refs[7 + n]
    me_ea, parity = places(sizes)
    slots = Slots(sizes, kind_ref, cell_ref, node_ref, coupling_ref)
    disp = disp_ref[...].reshape(sizes["components"] * sizes["rows"], sizes["depth_z"])
    pack(sizes, slots, me_ea, parity, disp, enr_ref[...], outs, part_ref)
    own_ref[...] = part_ref[me_ea]


def step_kernel(sizes, last, *refs):
    n = sizes["messages"]
    disp_ref, enr_ref, kind_ref, cell_ref, node_ref, coupling_ref = refs[:6]
    shift_ref, diag_ref, off_ref, own_ref = refs[6:10]
    got = split_outs(sizes, refs[10 : 10 + n])
    rest = refs[10 + n :]
    me_ea, parity = places(sizes)
    slots = Slots(sizes, kind_ref, cell_ref, node_ref, coupling_ref)
    rows, dz, comps = sizes["rows"], sizes["depth_z"], sizes["components"]
    disp = disp_ref[...].reshape(comps * rows, dz)
    enriched = enr_ref[...]
    shift = shift_ref[...].reshape(rows, dz)
    if last:
        moment_refs = rest[: ITERS - 1]
        next_disp_ref, next_enr_ref, sent_ref, held_ref = rest[ITERS - 1 :]
    else:
        outs = split_outs(sizes, rest[:n])
        next_disp_ref, next_enr_ref, next_own_ref, moments_ref, part_ref, held_ref = rest[n:]
    following = apply(
        sizes, slots, me_ea, parity, disp, enriched, shift, (diag_ref, off_ref), got, own_ref[...], held_ref
    )
    next_disp_ref[...] = following[0].reshape(next_disp_ref.shape)
    next_enr_ref[...] = following[1]
    here = (disp, enriched)
    if last:
        rows_of = [ref[j : j + 1] for ref in moment_refs for j in range(2)]
        rows_of += [partial_product(here, here), partial_product(here, following)]
        row = iota((8, dz), 0)
        table = jnp.zeros((8, dz), F32)
        for j, line in enumerate(rows_of):
            table = jnp.where(row == j, line, table)
        sums = jnp.sum(table, axis=1, keepdims=True)
        spread = jnp.where(iota((8, dz), 1) == row, sums, 0.0)
        sent_ref[...] = jnp.broadcast_to(jnp.sum(spread, axis=0, keepdims=True)[None], sent_ref.shape)
    else:
        pack(sizes, slots, me_ea, parity, following[0], following[1], outs, part_ref)
        next_own_ref[...] = part_ref[me_ea]
        moments_ref[0:1] = partial_product(here, here)
        moments_ref[1:2] = partial_product(here, following)


def coefficients(moments):
    def product(first, second):
        total = 0.0
        for i, a in enumerate(first):
            for j, b in enumerate(second):
                total = total + a * b * moments[i + j]
        return total

    def image(vector):
        out = [CENTRE * a for a in vector] + [0.0]
        return [a + (SPREAD * vector[i - 1] if i else 0.0) for i, a in enumerate(out)]

    def combine(first, factor, second):
        length = max(len(first), len(second))
        out = []
        for i in range(length):
            a = first[i] if i < len(first) else None
            b = factor * second[i] if i < len(second) else None
            out.append(b if a is None else a if b is None else a + b)
        return out

    one = jnp.ones_like(moments[0])
    solution, residual, direction = [], [one], [one]
    norm_now = moments[0]
    for iteration in range(ITERS):
        along = image(direction)
        alpha = norm_now / product(direction, along)
        solution = combine(solution, alpha, direction)
        residual = combine(residual, -alpha, along)
        if iteration + 1 < ITERS:
            norm_next = product(residual, residual)
            direction = combine(residual, norm_next / norm_now, direction)
            norm_now = norm_next
    return solution, residual


def final_kernel(sizes, *refs):
    sums_ref = refs[0]
    disps, enrs = refs[1 : 2 + ITERS], refs[2 + ITERS : 3 + 2 * ITERS]
    x_disp, r_disp, x_enr, r_enr = refs[3 + 2 * ITERS :]
    row = jnp.sum(sums_ref[...], axis=0)
    lanes = row.shape[1]
    moments = jnp.sum(jnp.where(iota((8, lanes), 0) == iota((8, lanes), 1), row, 0.0), axis=1, keepdims=True)
    solution, residual = coefficients([moments[j : j + 1] for j in range(2 * ITERS)])

    def mix(factors, vectors, shape):
        total = None
        for factor, ref in zip(factors, vectors):
            value = ref[...]
            term = jnp.broadcast_to(factor.reshape((1,) * value.ndim), value.shape) * value
            total = term if total is None else total + term
        return total

    x_disp[...] = mix(solution, disps, None)
    r_disp[...] = mix(residual, disps, None)
    x_enr[...] = mix(solution, enrs, None)
    r_enr[...] = mix(residual, enrs, None)


def struct(*shape):
    return jax.ShapeDtypeStruct(shape, F32)


def body(
    load_displacement,
    load_enriched,
    stiffness_shift,
    enriched_diag,
    enriched_off,
    coupling,
    slot_kind,
    slot_cell,
    slot_node,
):
    comps, dx, dy, dz = load_displacement.shape
    ne, nodes = load_enriched.shape
    owners = slot_kind.shape[1]
    counts = {axis: lax.axis_size(axis) for axis in AXES}
    perms_x = [p for p in (swap_pairs(counts["gx"], 0), swap_pairs(counts["gx"], 1)) if p]
    perms_y = [p for p in (swap_pairs(counts["gy"], 0), swap_pairs(counts["gy"], 1)) if p]
    perms_e = [partner_pairs(k, owners) for k in range(1, owners)]
    sizes = {
        "components": comps,
        "depth_x": dx,
        "depth_y": dy,
        "depth_z": dz,
        "rows": dx * dy,
        "enriched": ne,
        "nodes": nodes,
        "x_swaps": len(perms_x),
        "y_swaps": len(perms_y),
        "others": len(perms_e),
        "messages": len(perms_x) + len(perms_y) + len(perms_e),
    }
    devices = counts["gx"] * counts["gy"] * counts["ea"]
    wide = max(nodes, comps * dx * dy)
    message_shapes = (
        [struct(comps, dy, dz)] * len(perms_x)
        + [struct(comps * dx, dz)] * len(perms_y)
        + [struct(2 * ne + 2, wide)] * len(perms_e)
    )
    routes = [("gx", p) for p in perms_x] + [("gy", p) for p in perms_y] + [("ea", p) for p in perms_e]
    slot_args = (slot_kind, slot_cell, slot_node, coupling)
    part_scratch = pltpu.VMEM((owners, ne, nodes), F32)
    held_scratch = pltpu.VMEM((owners, 2 * ne + 2, wide), F32)

    def exchange(messages):
        return [lax.ppermute(m, axis, pairs) for m, (axis, pairs) in zip(messages, routes)]

    disps, enrs, moments = [load_displacement], [load_enriched], []
    outs = pl.pallas_call(
        functools.partial(first_kernel, sizes),
        out_shape=message_shapes + [struct(ne, nodes)],
        scratch_shapes=[part_scratch],
        name="first",
    )(load_displacement, load_enriched, *slot_args)
    messages, own = outs[:-1], outs[-1]
    for iteration in range(ITERS):
        last = iteration + 1 == ITERS
        received = exchange(messages)
        args = (disps[-1], enrs[-1], *slot_args, stiffness_shift, enriched_diag, enriched_off, own, *received)
        vectors = [struct(comps, dx, dy, dz), struct(ne, nodes)]
        if last:
            outs = pl.pallas_call(
                functools.partial(step_kernel, sizes, True),
                out_shape=vectors + [struct(devices, 1, dz)],
                scratch_shapes=[held_scratch],
                name="last",
            )(*args, *moments)
            disps.append(outs[0])
            enrs.append(outs[1])
            sent = outs[2]
        else:
            outs = pl.pallas_call(
                functools.partial(step_kernel, sizes, False),
                out_shape=message_shapes + vectors + [struct(ne, nodes), struct(2, dz)],
                scratch_shapes=[part_scratch, held_scratch],
                name="step",
            )(*args)
            messages = outs[: sizes["messages"]]
            disp, enr, own, moment = outs[sizes["messages"] :]
            disps.append(disp)
            enrs.append(enr)
            moments.append(moment)
    sums = lax.all_to_all(sent, AXES, 0, 0, tiled=True)
    return pl.pallas_call(
        functools.partial(final_kernel, sizes),
        out_shape=[struct(comps, dx, dy, dz)] * 2 + [struct(ne, nodes)] * 2,
        name="final",
    )(sums, *disps, *enrs)


def solution(mesh):
    placed = (
        P(None, "gx", "gy", "ea"),
        P(None, ("gx", "gy", "ea")),
        P("gx", "gy", "ea"),
        P(None, ("gx", "gy", "ea")),
        P(None, None, ("gx", "gy", "ea")),
        P(None, None, ("gx", "gy", "ea")),
        P(("gx", "gy", "ea"), None, None),
        P(("gx", "gy", "ea"), None, None),
        P(("gx", "gy", "ea"), None, None),
    )
    return jax.shard_map(
        body,
        mesh=mesh,
        in_specs=placed,
        out_specs=(
            P(None, "gx", "gy", "ea"),
            P(None, "gx", "gy", "ea"),
            P(None, ("gx", "gy", "ea")),
            P(None, ("gx", "gy", "ea")),
        ),
        check_vma=False,
    )
```

```python
import functools

import jax
import jax.numpy as jnp
from jax import lax
from jax.experimental import pallas as pl
from jax.experimental.pallas import tpu as pltpu
from jax.sharding import PartitionSpec as P

ITERS = 3
CENTRE = 11.0
SPREAD = 8.0
AXES = ("gx", "gy", "ea")
LOCAL_FLOPS = 2000000
F32 = jnp.float32
BF16 = jnp.bfloat16


def swap_pairs(count, first):
    pairs = []
    for i in range(first, count - 1, 2):
        pairs += [(i, i + 1), (i + 1, i)]
    return pairs


def partner(me, step, count):
    return me ^ step if count & (count - 1) == 0 else lax.rem(me + step, count)


def slot_of(me, owner, count):
    return me ^ owner if count & (count - 1) == 0 else lax.rem(me - owner + count, count)


def partner_pairs(step, count):
    if count & (count - 1) == 0:
        return [(i, i ^ step) for i in range(count)]
    return [(i, (i + step) % count) for i in range(count)]


def halves(value):
    high = value.astype(BF16)
    low = (value - high.astype(F32)).astype(BF16)
    return high, low


def iota(shape, dim):
    return lax.broadcasted_iota(jnp.int32, shape, dim)


def one_hot(flag):
    return jnp.where(flag, 1.0, 0.0).astype(BF16)


def dot(left, right, dims):
    return lax.dot_general(left, right, (dims, ((), ())), preferred_element_type=F32)


NN = ((1,), (0,))
NT = ((1,), (1,))
TN = ((0,), (0,))


class Hots:
    def __init__(self, refs):
        self.weights, self.row_hot, self.z_hot, self.node_hot = refs

    @staticmethod
    def shapes(sizes):
        total = sizes["owners"] * sizes["capacity"]
        return [
            struct(sizes["components"], sizes["enriched"], total),
            struct(sizes["rows"], total),
            struct(sizes["depth_z"], total, dtype=BF16),
            struct(sizes["owners"], sizes["nodes"], sizes["capacity"], dtype=BF16),
        ]

    def fill(self, sizes, kind_ref, cell_ref, node_ref, coupling_ref):
        owners, capacity = sizes["owners"], sizes["capacity"]
        total = owners * capacity
        rows, depth_z = sizes["rows"], sizes["depth_z"]
        cells = jnp.concatenate([cell_ref[0, o : o + 1, :] for o in range(owners)], axis=1)
        kinds = jnp.concatenate([kind_ref[0, o : o + 1, :] for o in range(owners)], axis=1)
        cell_row = cells // depth_z
        cell_z = cells - cell_row * depth_z
        self.row_hot[...] = jnp.where(iota((rows, total), 0) == cell_row, 1.0, 0.0)
        self.z_hot[...] = one_hot(iota((depth_z, total), 0) == cell_z)
        for o in range(owners):
            self.node_hot[o] = one_hot(
                iota((sizes["nodes"], capacity), 0) == node_ref[0, o : o + 1, :]
            )
        heaviside = jnp.where(kinds >= 1, 1.0, 0.0)
        tip = jnp.where(kinds == 2, 1.0, 0.0)
        masks = jnp.where(iota((sizes["enriched"], total), 0) < 3, heaviside, tip)
        for p in range(sizes["components"]):
            self.weights[p] = coupling_ref[p] * masks


def pack(sizes, hots, me_ea, parity, disp, enriched, outs, part_ref):
    comps, dx, dy, dz, rows, ne = (
        sizes[k] for k in ("components", "depth_x", "depth_y", "depth_z", "rows", "enriched")
    )
    owners, capacity = sizes["owners"], sizes["capacity"]
    grid = disp.reshape(comps, dx, dy, dz)
    even_x, even_y = parity
    first_x, last_x = grid[:, 0], grid[:, dx - 1]
    for j, out in enumerate(outs["gx"]):
        out[...] = jnp.where(even_x == (j == 0), last_x, first_x)
    lines = disp.reshape(comps * dx, dy, dz)
    for j, out in enumerate(outs["gy"]):
        out[...] = jnp.where(even_y == (j == 0), lines[:, dy - 1], lines[:, 0])
    high, low = halves(disp)
    columns = dot(jnp.concatenate([high, low], axis=0), hots.z_hot[...], NN)
    columns = columns[: comps * rows] + columns[comps * rows :]
    to_nodes = None
    for p in range(comps):
        picked = jnp.sum(hots.row_hot[...] * columns[p * rows : (p + 1) * rows], axis=0, keepdims=True)
        term = hots.weights[p] * picked
        to_nodes = term if to_nodes is None else to_nodes + term
    node_high, node_low = halves(to_nodes)
    for o in range(owners):
        block = slice(o * capacity, (o + 1) * capacity)
        part_ref[o] = dot(node_high[:, block], hots.node_hot[o], NT) + dot(
            node_low[:, block], hots.node_hot[o], NT
        )
    edge = one_hot(
        (iota((8, dz), 0) == 0) & (iota((8, dz), 1) == 0)
        | (iota((8, dz), 0) == 1) & (iota((8, dz), 1) == dz - 1)
    )
    faces = dot(edge, high, NT) + dot(edge, low, NT)
    for k, out in enumerate(outs["ea"]):
        out[:ne] = enriched
        out[ne + 1 : 2 * ne + 1] = part_ref[partner(me_ea, k + 1, owners)]
        out[ne : ne + 1, : comps * rows] = faces[0:1]
        out[2 * ne + 1 : 2 * ne + 2, : comps * rows] = faces[1:2]


def slots_to_cells(sizes, hots, values):
    comps, rows = sizes["components"], sizes["rows"]
    spread_high, spread_low = [], []
    for p in range(comps):
        to_cells = jnp.sum(hots.weights[p] * values, axis=0, keepdims=True)
        c_high, c_low = halves(to_cells)
        spread_high.append((hots.row_hot[...] * c_high.astype(F32)).astype(BF16))
        spread_low.append((hots.row_hot[...] * c_low.astype(F32)).astype(BF16))
    added = dot(jnp.concatenate(spread_high + spread_low, axis=0), hots.z_hot[...], NT)
    return added[: comps * rows] + added[comps * rows :]


def apply_local(sizes, disp, enriched, own_part, scale, stiff_ref):
    comps, dx, dy, dz, rows, ne = (
        sizes[k] for k in ("components", "depth_x", "depth_y", "depth_z", "rows", "enriched")
    )
    grid = disp.reshape(comps, dx, dy, dz)
    no_x = jnp.zeros((comps, 1, dy, dz), F32)
    beside = jnp.concatenate([grid[:, 1:], no_x], axis=1) + jnp.concatenate([no_x, grid[:, :-1]], axis=1)
    beside = beside.reshape(comps * rows, dz)
    total_rows = comps * rows
    y_place = iota((total_rows, dz), 0) % dy
    beside = beside + jnp.where(y_place == 0, 0.0, pltpu.roll(disp, 1, 0))
    beside = beside + jnp.where(y_place == dy - 1, 0.0, pltpu.roll(disp, total_rows - 1, 0))
    z_place = iota((total_rows, dz), 1)
    beside = beside + jnp.where(z_place == 0, 0.0, pltpu.roll(disp, 1, 1))
    beside = beside + jnp.where(z_place == dz - 1, 0.0, pltpu.roll(disp, dz - 1, 1))
    scaled = (scale[None] * disp.reshape(comps, rows, dz)).reshape(total_rows, dz)
    pushed = own_part
    for q in range(ne):
        pushed = pushed + stiff_ref[q] * enriched[q : q + 1]
    return scaled - beside, pushed


def combine(sizes, hots, me_ea, parity, local, enriched, got, held_ref):
    comps, dx, dy, dz, rows, ne = (
        sizes[k] for k in ("components", "depth_x", "depth_y", "depth_z", "rows", "enriched")
    )
    owners = sizes["owners"]
    total_rows = comps * rows
    local_disp, local_enriched = local
    held_ref[0, :ne] = enriched
    for k, ref in enumerate(got["ea"]):
        held_ref[k + 1] = ref[...]
    values = []
    for o in range(owners):
        w_high, w_low = halves(held_ref[slot_of(me_ea, o, owners), :ne, :])
        values.append(dot(w_high, hots.node_hot[o], NN) + dot(w_low, hots.node_hot[o], NN))
    added = slots_to_cells(sizes, hots, jnp.concatenate(values, axis=1))
    even_x, even_y = parity
    zero_x = jnp.zeros((comps, dy, dz), F32)
    zero_y = jnp.zeros((comps * dx, dz), F32)
    x_a = got["gx"][0][...] if len(got["gx"]) > 0 else zero_x
    x_b = got["gx"][1][...] if len(got["gx"]) > 1 else zero_x
    y_a = got["gy"][0][...] if len(got["gy"]) > 0 else zero_y
    y_b = got["gy"][1][...] if len(got["gy"]) > 1 else zero_y
    below_x = jnp.where(even_x, x_b, x_a)
    above_x = jnp.where(even_x, x_a, x_b)
    below_y = jnp.where(even_y, y_b, y_a)
    above_y = jnp.where(even_y, y_a, y_b)
    no_x = jnp.zeros((comps, dx - 2, dy, dz), F32)
    beside = jnp.concatenate([below_x[:, None], no_x, above_x[:, None]], axis=1).reshape(total_rows, dz)
    y_place = iota((total_rows, dz), 0) % dy
    spread_y = (comps * dx, dy, dz)
    low_y = jnp.broadcast_to(below_y[:, None, :], spread_y).reshape(total_rows, dz)
    high_y = jnp.broadcast_to(above_y[:, None, :], spread_y).reshape(total_rows, dz)
    beside = beside + jnp.where(y_place == 0, low_y, jnp.where(y_place == dy - 1, high_y, 0.0))
    below = jnp.maximum(me_ea - 1, 0)
    above = jnp.minimum(me_ea + 1, owners - 1)
    low_z = held_ref[slot_of(me_ea, below, owners), 2 * ne + 1 : 2 * ne + 2, :total_rows]
    high_z = held_ref[slot_of(me_ea, above, owners), ne : ne + 1, :total_rows]
    low_z = jnp.where(me_ea > 0, low_z, 0.0)
    high_z = jnp.where(me_ea < owners - 1, high_z, 0.0)
    line = iota((8, total_rows), 0)
    lows, highs = halves(low_z), halves(high_z)
    sides = jnp.zeros((8, total_rows), F32)
    for j, part in enumerate((lows[0], lows[1], highs[0], highs[1])):
        sides = jnp.where(line == j, part.astype(F32), sides)
    edge_row, edge_lane = iota((8, dz), 0), iota((8, dz), 1)
    edge = one_hot(
        (edge_row < 2) & (edge_lane == 0) | (edge_row >= 2) & (edge_row < 4) & (edge_lane == dz - 1)
    )
    beside = beside + dot(sides.astype(BF16), edge, TN)
    next_disp = (local_disp - beside + added) * (1.0 / SPREAD)
    node_terms = local_enriched
    for ref in got["ea"]:
        node_terms = node_terms + ref[ne + 1 : 2 * ne + 1]
    return next_disp, node_terms * (1.0 / SPREAD)


def partial_product(first, second):
    grid = first[0] * second[0]
    total = jnp.sum(grid, axis=0, keepdims=True)
    nodes = jnp.sum(first[1] * second[1], axis=0, keepdims=True)
    lanes = grid.shape[1]
    for j in range(nodes.shape[1] // lanes):
        total = total + nodes[:, j * lanes : (j + 1) * lanes]
    return total


def places(sizes):
    return lax.axis_index("ea"), (lax.axis_index("gx") % 2 == 0, lax.axis_index("gy") % 2 == 0)


def split_outs(sizes, refs):
    n_x, n_y, n_e = sizes["x_swaps"], sizes["y_swaps"], sizes["others"]
    return {"gx": refs[:n_x], "gy": refs[n_x : n_x + n_y], "ea": refs[n_x + n_y : n_x + n_y + n_e]}


def first_kernel(sizes, *refs):
    disp_ref, enr_ref, kind_ref, cell_ref, node_ref, coupling_ref = refs[:6]
    n = sizes["messages"]
    outs = split_outs(sizes, refs[6 : 6 + n])
    own_ref, disp_copy, enr_copy = refs[6 + n : 9 + n]
    hots = Hots(refs[9 + n : 13 + n])
    part_ref = refs[13 + n]
    me_ea, parity = places(sizes)
    hots.fill(sizes, kind_ref, cell_ref, node_ref, coupling_ref)
    disp = disp_ref[...].reshape(sizes["components"] * sizes["rows"], sizes["depth_z"])
    enriched = enr_ref[...]
    pack(sizes, hots, me_ea, parity, disp, enriched, outs, part_ref)
    own_ref[...] = part_ref[me_ea]
    disp_copy[...] = disp_ref[...]
    enr_copy[...] = enriched


def local_kernel(sizes, first, *refs):
    disp_ref, enr_ref = refs[:2]
    rows, dz = sizes["rows"], sizes["depth_z"]
    ne = sizes["enriched"]
    if first:
        shift_ref, diag_ref, off_ref, own_ref = refs[2:6]
        local_disp, local_enr, moment_ref, scale_ref, stiff_ref = refs[6:]
        scale_ref[...] = (6.0 - CENTRE) + shift_ref[...].reshape(rows, dz)
        diag = diag_ref[...] - CENTRE
        row = iota(diag.shape, 0)
        for q in range(ne):
            turned = jnp.concatenate([off_ref[p, q : q + 1] for p in range(ne)], axis=0)
            stiff_ref[q] = jnp.where(row == q, diag, 0.5 * (off_ref[q] + turned))
    else:
        own_ref, scale_ref, stiff_ref, local_disp, local_enr, moment_ref = refs[2:]
    disp = disp_ref[...].reshape(sizes["components"] * rows, dz)
    enriched = enr_ref[...]
    pushed = apply_local(sizes, disp, enriched, own_ref[...], scale_ref[...], stiff_ref)
    local_disp[...], local_enr[...] = pushed
    here = (disp, enriched)
    moment_ref[...] = partial_product(here, here)


def combine_kernel(sizes, last, *refs):
    n = sizes["messages"]
    local_disp, local_enr, disp_ref, enr_ref = refs[:4]
    hots = Hots(refs[4:8])
    got = split_outs(sizes, refs[8 : 8 + n])
    rest = refs[8 + n :]
    me_ea, parity = places(sizes)
    rows, dz, comps = sizes["rows"], sizes["depth_z"], sizes["components"]
    disp = disp_ref[...].reshape(comps * rows, dz)
    enriched = enr_ref[...]
    if last:
        moment_refs = rest[: 2 * ITERS - 1]
        next_disp_ref, next_enr_ref, sent_ref, held_ref = rest[2 * ITERS - 1 :]
    else:
        outs = split_outs(sizes, rest[:n])
        next_disp_ref, next_enr_ref, next_own_ref, moment_ref, part_ref, held_ref = rest[n:]
    local = (local_disp[...], local_enr[...])
    following = combine(sizes, hots, me_ea, parity, local, enriched, got, held_ref)
    next_disp_ref[...] = following[0].reshape(next_disp_ref.shape)
    next_enr_ref[...] = following[1]
    product = partial_product((disp, enriched), following)
    if last:
        row = iota((8, dz), 0)
        table = jnp.where(row == 2 * ITERS - 1, product, 0.0)
        for j, ref in enumerate(moment_refs):
            table = jnp.where(row == j, ref[...], table)
        sums = jnp.sum(table, axis=1, keepdims=True)
        spread = jnp.where(iota((8, dz), 1) == row, sums, 0.0)
        sent_ref[...] = jnp.broadcast_to(jnp.sum(spread, axis=0, keepdims=True)[None], sent_ref.shape)
    else:
        pack(sizes, hots, me_ea, parity, following[0], following[1], outs, part_ref)
        next_own_ref[...] = part_ref[me_ea]
        moment_ref[...] = product


def coefficients(moments):
    def product(first, second):
        total = 0.0
        for i, a in enumerate(first):
            for j, b in enumerate(second):
                total = total + a * b * moments[i + j]
        return total

    def image(vector):
        out = [CENTRE * a for a in vector] + [0.0]
        return [a + (SPREAD * vector[i - 1] if i else 0.0) for i, a in enumerate(out)]

    def combine(first, factor, second):
        length = max(len(first), len(second))
        out = []
        for i in range(length):
            a = first[i] if i < len(first) else None
            b = factor * second[i] if i < len(second) else None
            out.append(b if a is None else a if b is None else a + b)
        return out

    one = jnp.ones_like(moments[0])
    solution, residual, direction = [], [one], [one]
    norm_now = moments[0]
    for iteration in range(ITERS):
        along = image(direction)
        alpha = norm_now / product(direction, along)
        solution = combine(solution, alpha, direction)
        residual = combine(residual, -alpha, along)
        if iteration + 1 < ITERS:
            norm_next = product(residual, residual)
            direction = combine(residual, norm_next / norm_now, direction)
            norm_now = norm_next
    return solution, residual


def final_kernel(sizes, *refs):
    sums_ref = refs[0]
    disps, enrs = refs[1 : 2 + ITERS], refs[2 + ITERS : 3 + 2 * ITERS]
    x_disp, r_disp, x_enr, r_enr = refs[3 + 2 * ITERS :]
    row = jnp.sum(sums_ref[...], axis=0)
    lanes = row.shape[1]
    moments = jnp.sum(jnp.where(iota((8, lanes), 0) == iota((8, lanes), 1), row, 0.0), axis=1, keepdims=True)
    solution, residual = coefficients([moments[j : j + 1] for j in range(2 * ITERS)])

    def mix(factors, vectors, shape):
        total = None
        for factor, ref in zip(factors, vectors):
            value = ref[...]
            term = jnp.broadcast_to(factor.reshape((1,) * value.ndim), value.shape) * value
            total = term if total is None else total + term
        return total

    x_disp[...] = mix(solution, disps, None)
    r_disp[...] = mix(residual, disps, None)
    x_enr[...] = mix(solution, enrs, None)
    r_enr[...] = mix(residual, enrs, None)


def struct(*shape, dtype=F32):
    return pltpu.VMEM(shape, dtype)


def call(kernel, out_shape, name, scratch=(), flops=0):
    cost = pl.CostEstimate(flops=flops, bytes_accessed=0, transcendentals=0)
    run = pl.pallas_call(
        kernel, out_shape=out_shape, scratch_shapes=list(scratch), name=name, cost_estimate=cost
    )

    def with_args(given, kept):
        return run(*given, *(pltpu.with_memory_space_constraint(a, pltpu.VMEM) for a in kept))

    return with_args


def body(
    load_displacement,
    load_enriched,
    stiffness_shift,
    enriched_diag,
    enriched_off,
    coupling,
    slot_kind,
    slot_cell,
    slot_node,
):
    comps, dx, dy, dz = load_displacement.shape
    ne, nodes = load_enriched.shape
    owners = slot_kind.shape[1]
    counts = {axis: lax.axis_size(axis) for axis in AXES}
    perms_x = [p for p in (swap_pairs(counts["gx"], 0), swap_pairs(counts["gx"], 1)) if p]
    perms_y = [p for p in (swap_pairs(counts["gy"], 0), swap_pairs(counts["gy"], 1)) if p]
    perms_e = [partner_pairs(k, owners) for k in range(1, owners)]
    sizes = {
        "components": comps,
        "depth_x": dx,
        "depth_y": dy,
        "depth_z": dz,
        "rows": dx * dy,
        "enriched": ne,
        "nodes": nodes,
        "owners": owners,
        "capacity": slot_kind.shape[2],
        "x_swaps": len(perms_x),
        "y_swaps": len(perms_y),
        "others": len(perms_e),
        "messages": len(perms_x) + len(perms_y) + len(perms_e),
    }
    devices = counts["gx"] * counts["gy"] * counts["ea"]
    wide = max(nodes, comps * dx * dy)
    message_shapes = (
        [struct(comps, dy, dz)] * len(perms_x)
        + [struct(comps * dx, dz)] * len(perms_y)
        + [struct(2 * ne + 2, wide)] * len(perms_e)
    )
    routes = [("gx", p) for p in perms_x] + [("gy", p) for p in perms_y] + [("ea", p) for p in perms_e]
    part_scratch = pltpu.VMEM((owners, ne, nodes), F32)
    held_scratch = pltpu.VMEM((owners, 2 * ne + 2, wide), F32)
    vector = [struct(comps, dx, dy, dz), struct(ne, nodes)]
    flat_vector = [struct(comps * dx * dy, dz), struct(ne, nodes)]
    moment = struct(1, dz)
    n = sizes["messages"]

    outs = call(
        functools.partial(first_kernel, sizes),
        message_shapes + [struct(ne, nodes)] + vector + Hots.shapes(sizes),
        "first",
        [part_scratch],
    )((load_displacement, load_enriched, slot_kind, slot_cell, slot_node, coupling), ())
    messages, own, disps, enrs, hots = outs[:n], outs[n], [outs[n + 1]], [outs[n + 2]], outs[n + 3 :]
    moments, fixed = [], None
    for iteration in range(ITERS):
        received = [lax.ppermute(m, axis, pairs) for m, (axis, pairs) in zip(messages, routes)]
        here = (disps[-1], enrs[-1], own)
        first, last = iteration == 0, iteration + 1 == ITERS
        shapes = flat_vector + [moment]
        if first:
            shapes = shapes + [struct(dx * dy, dz), struct(ne, ne, nodes)]
        run = call(functools.partial(local_kernel, sizes, first), shapes, "local", flops=LOCAL_FLOPS)
        if first:
            given = (load_displacement, load_enriched)
            outs = run((*given, stiffness_shift, enriched_diag, enriched_off), (own,))
            fixed = outs[3:]
        else:
            outs = run((), (*here, *fixed))
        local = outs[:2]
        moments.append(outs[2])
        kept = (*local, *here[:2], *hots, *received)
        if last:
            disp, enr, sent = call(
                functools.partial(combine_kernel, sizes, True),
                vector + [struct(devices, 1, dz)],
                "last",
                [held_scratch],
            )((), (*kept, *moments))
        else:
            outs = call(
                functools.partial(combine_kernel, sizes, False),
                message_shapes + vector + [struct(ne, nodes), moment],
                "combine",
                [part_scratch, held_scratch],
            )((), kept)
            messages = outs[:n]
            disp, enr, own, product = outs[n:]
            moments.append(product)
        disps.append(disp)
        enrs.append(enr)
    sums = lax.all_to_all(sent, AXES, 0, 0, tiled=True)
    outs = [jax.ShapeDtypeStruct(a.shape, F32) for a in (disps[0], disps[0], enrs[0], enrs[0])]
    return call(functools.partial(final_kernel, sizes), outs, "final")((), (sums, *disps, *enrs))


def solution(mesh):
    placed = (
        P(None, "gx", "gy", "ea"),
        P(None, ("gx", "gy", "ea")),
        P("gx", "gy", "ea"),
        P(None, ("gx", "gy", "ea")),
        P(None, None, ("gx", "gy", "ea")),
        P(None, None, ("gx", "gy", "ea")),
        P(("gx", "gy", "ea"), None, None),
        P(("gx", "gy", "ea"), None, None),
        P(("gx", "gy", "ea"), None, None),
    )
    return jax.shard_map(
        body,
        mesh=mesh,
        in_specs=placed,
        out_specs=(
            P(None, "gx", "gy", "ea"),
            P(None, "gx", "gy", "ea"),
            P(None, ("gx", "gy", "ea")),
            P(None, ("gx", "gy", "ea")),
        ),
        check_vma=False,
    )
```

```python
import functools
import itertools
import math

import jax
import jax.numpy as jnp
from jax import lax
from jax.experimental import pallas as pl
from jax.experimental.pallas import tpu as pltpu
from jax.sharding import PartitionSpec as P

ITERS = 3
CENTRE = 11.0
SPREAD = 8.0
AXES = ("gx", "gy", "ea")
LOCAL_FLOPS = 2000000
F32 = jnp.float32
BF16 = jnp.bfloat16


def swap_pairs(counts, axis, first):
    count, at = counts[axis], AXES.index(axis)
    if first + 1 >= count:
        return []
    sizes = [counts[a] for a in AXES]
    pairs = []
    for place in itertools.product(*(range(n) for n in sizes)):
        other = list(place)
        mate = first + ((place[at] - first) ^ 1)
        if place[at] >= first and mate < count:
            other[at] = mate
        elif sizes[-1] % 2 == 0:
            other[-1] = place[-1] ^ 1
        flat = [sum(p * math.prod(sizes[j + 1 :]) for j, p in enumerate(x)) for x in (place, other)]
        pairs.append(tuple(flat))
    return pairs


def partner(me, step, count):
    return me ^ step if count & (count - 1) == 0 else lax.rem(me + step, count)


def slot_of(me, owner, count):
    return me ^ owner if count & (count - 1) == 0 else lax.rem(me - owner + count, count)


def partner_pairs(step, count):
    if count & (count - 1) == 0:
        return [(i, i ^ step) for i in range(count)]
    return [(i, (i + step) % count) for i in range(count)]


def halves(value):
    high = value.astype(BF16)
    low = (value - high.astype(F32)).astype(BF16)
    return high, low


def iota(shape, dim):
    return lax.broadcasted_iota(jnp.int32, shape, dim)


def one_hot(flag):
    return jnp.where(flag, 1.0, 0.0).astype(BF16)


def dot(left, right, dims):
    return lax.dot_general(left, right, (dims, ((), ())), preferred_element_type=F32)


NN = ((1,), (0,))
NT = ((1,), (1,))
TN = ((0,), (0,))


class Hots:
    def __init__(self, refs):
        self.weights, self.row_hot, self.z_hot, self.node_hot = refs

    @staticmethod
    def shapes(sizes):
        total = sizes["owners"] * sizes["capacity"]
        return [
            struct(sizes["components"], sizes["enriched"], total),
            struct(sizes["rows"], total),
            struct(sizes["depth_z"], total, dtype=BF16),
            struct(sizes["owners"], sizes["nodes"], sizes["capacity"], dtype=BF16),
        ]

    def fill(self, sizes, kind_ref, cell_ref, node_ref, coupling_ref):
        owners, capacity = sizes["owners"], sizes["capacity"]
        total = owners * capacity
        rows, depth_z = sizes["rows"], sizes["depth_z"]
        cells = jnp.concatenate([cell_ref[0, o : o + 1, :] for o in range(owners)], axis=1)
        kinds = jnp.concatenate([kind_ref[0, o : o + 1, :] for o in range(owners)], axis=1)
        cell_row = cells // depth_z
        cell_z = cells - cell_row * depth_z
        self.row_hot[...] = jnp.where(iota((rows, total), 0) == cell_row, 1.0, 0.0)
        self.z_hot[...] = one_hot(iota((depth_z, total), 0) == cell_z)
        for o in range(owners):
            self.node_hot[o] = one_hot(
                iota((sizes["nodes"], capacity), 0) == node_ref[0, o : o + 1, :]
            )
        heaviside = jnp.where(kinds >= 1, 1.0, 0.0)
        tip = jnp.where(kinds == 2, 1.0, 0.0)
        masks = jnp.where(iota((sizes["enriched"], total), 0) < 3, heaviside, tip)
        for p in range(sizes["components"]):
            self.weights[p] = coupling_ref[p] * masks


def pack(sizes, hots, me_ea, parity, disp, enriched, outs, part_ref):
    comps, dx, dy, dz, rows, ne = (
        sizes[k] for k in ("components", "depth_x", "depth_y", "depth_z", "rows", "enriched")
    )
    owners, capacity = sizes["owners"], sizes["capacity"]
    grid = disp.reshape(comps, dx, dy, dz)
    even_x, even_y = parity
    first_x, last_x = grid[:, 0], grid[:, dx - 1]
    for j, out in enumerate(outs["gx"]):
        out[...] = jnp.where(even_x == (j == 0), last_x, first_x)
    lines = disp.reshape(comps * dx, dy, dz)
    for j, out in enumerate(outs["gy"]):
        out[...] = jnp.where(even_y == (j == 0), lines[:, dy - 1], lines[:, 0])
    high, low = halves(disp)
    columns = dot(jnp.concatenate([high, low], axis=0), hots.z_hot[...], NN)
    columns = columns[: comps * rows] + columns[comps * rows :]
    to_nodes = None
    for p in range(comps):
        picked = jnp.sum(hots.row_hot[...] * columns[p * rows : (p + 1) * rows], axis=0, keepdims=True)
        term = hots.weights[p] * picked
        to_nodes = term if to_nodes is None else to_nodes + term
    node_high, node_low = halves(to_nodes)
    for o in range(owners):
        block = slice(o * capacity, (o + 1) * capacity)
        part_ref[o] = dot(node_high[:, block], hots.node_hot[o], NT) + dot(
            node_low[:, block], hots.node_hot[o], NT
        )
    edge = one_hot(
        (iota((8, dz), 0) == 0) & (iota((8, dz), 1) == 0)
        | (iota((8, dz), 0) == 1) & (iota((8, dz), 1) == dz - 1)
    )
    faces = dot(edge, high, NT) + dot(edge, low, NT)
    for k, out in enumerate(outs["ea"]):
        out[:ne] = enriched
        out[ne + 1 : 2 * ne + 1] = part_ref[partner(me_ea, k + 1, owners)]
        out[ne : ne + 1, : comps * rows] = faces[0:1]
        out[2 * ne + 1 : 2 * ne + 2, : comps * rows] = faces[1:2]


def slots_to_cells(sizes, hots, values):
    comps, rows = sizes["components"], sizes["rows"]
    spread_high, spread_low = [], []
    for p in range(comps):
        to_cells = jnp.sum(hots.weights[p] * values, axis=0, keepdims=True)
        c_high, c_low = halves(to_cells)
        spread_high.append((hots.row_hot[...] * c_high.astype(F32)).astype(BF16))
        spread_low.append((hots.row_hot[...] * c_low.astype(F32)).astype(BF16))
    added = dot(jnp.concatenate(spread_high + spread_low, axis=0), hots.z_hot[...], NT)
    return added[: comps * rows] + added[comps * rows :]


def apply_local(sizes, disp, enriched, own_part, scale, stiff_ref):
    comps, dx, dy, dz, rows, ne = (
        sizes[k] for k in ("components", "depth_x", "depth_y", "depth_z", "rows", "enriched")
    )
    grid = disp.reshape(comps, dx, dy, dz)
    no_x = jnp.zeros((comps, 1, dy, dz), F32)
    beside = jnp.concatenate([grid[:, 1:], no_x], axis=1) + jnp.concatenate([no_x, grid[:, :-1]], axis=1)
    beside = beside.reshape(comps * rows, dz)
    total_rows = comps * rows
    y_place = iota((total_rows, dz), 0) % dy
    beside = beside + jnp.where(y_place == 0, 0.0, pltpu.roll(disp, 1, 0))
    beside = beside + jnp.where(y_place == dy - 1, 0.0, pltpu.roll(disp, total_rows - 1, 0))
    z_place = iota((total_rows, dz), 1)
    beside = beside + jnp.where(z_place == 0, 0.0, pltpu.roll(disp, 1, 1))
    beside = beside + jnp.where(z_place == dz - 1, 0.0, pltpu.roll(disp, dz - 1, 1))
    scaled = (scale[None] * disp.reshape(comps, rows, dz)).reshape(total_rows, dz)
    pushed = own_part
    for q in range(ne):
        pushed = pushed + stiff_ref[q] * enriched[q : q + 1]
    return scaled - beside, pushed


def combine(sizes, hots, me_ea, parity, local, enriched, got, held_ref):
    comps, dx, dy, dz, rows, ne = (
        sizes[k] for k in ("components", "depth_x", "depth_y", "depth_z", "rows", "enriched")
    )
    owners = sizes["owners"]
    total_rows = comps * rows
    local_disp, local_enriched = local
    held_ref[0, :ne] = enriched
    for k, ref in enumerate(got["ea"]):
        held_ref[k + 1] = ref[...]
    values = []
    for o in range(owners):
        w_high, w_low = halves(held_ref[slot_of(me_ea, o, owners), :ne, :])
        values.append(dot(w_high, hots.node_hot[o], NN) + dot(w_low, hots.node_hot[o], NN))
    added = slots_to_cells(sizes, hots, jnp.concatenate(values, axis=1))
    even_x, even_y = parity
    zero_x = jnp.zeros((comps, dy, dz), F32)
    zero_y = jnp.zeros((comps * dx, dz), F32)
    x_a = got["gx"][0][...] if len(got["gx"]) > 0 else zero_x
    x_b = got["gx"][1][...] if len(got["gx"]) > 1 else zero_x
    y_a = got["gy"][0][...] if len(got["gy"]) > 0 else zero_y
    y_b = got["gy"][1][...] if len(got["gy"]) > 1 else zero_y
    (first_x, last_x), (first_y, last_y) = ends()
    below_x = jnp.where(first_x, 0.0, jnp.where(even_x, x_b, x_a))
    above_x = jnp.where(last_x, 0.0, jnp.where(even_x, x_a, x_b))
    below_y = jnp.where(first_y, 0.0, jnp.where(even_y, y_b, y_a))
    above_y = jnp.where(last_y, 0.0, jnp.where(even_y, y_a, y_b))
    no_x = jnp.zeros((comps, dx - 2, dy, dz), F32)
    beside = jnp.concatenate([below_x[:, None], no_x, above_x[:, None]], axis=1).reshape(total_rows, dz)
    y_place = iota((total_rows, dz), 0) % dy
    spread_y = (comps * dx, dy, dz)
    low_y = jnp.broadcast_to(below_y[:, None, :], spread_y).reshape(total_rows, dz)
    high_y = jnp.broadcast_to(above_y[:, None, :], spread_y).reshape(total_rows, dz)
    beside = beside + jnp.where(y_place == 0, low_y, jnp.where(y_place == dy - 1, high_y, 0.0))
    below = jnp.maximum(me_ea - 1, 0)
    above = jnp.minimum(me_ea + 1, owners - 1)
    low_z = held_ref[slot_of(me_ea, below, owners), 2 * ne + 1 : 2 * ne + 2, :total_rows]
    high_z = held_ref[slot_of(me_ea, above, owners), ne : ne + 1, :total_rows]
    low_z = jnp.where(me_ea > 0, low_z, 0.0)
    high_z = jnp.where(me_ea < owners - 1, high_z, 0.0)
    line = iota((8, total_rows), 0)
    lows, highs = halves(low_z), halves(high_z)
    sides = jnp.zeros((8, total_rows), F32)
    for j, part in enumerate((lows[0], lows[1], highs[0], highs[1])):
        sides = jnp.where(line == j, part.astype(F32), sides)
    edge_row, edge_lane = iota((8, dz), 0), iota((8, dz), 1)
    edge = one_hot(
        (edge_row < 2) & (edge_lane == 0) | (edge_row >= 2) & (edge_row < 4) & (edge_lane == dz - 1)
    )
    beside = beside + dot(sides.astype(BF16), edge, TN)
    next_disp = (local_disp - beside + added) * (1.0 / SPREAD)
    node_terms = local_enriched
    for ref in got["ea"]:
        node_terms = node_terms + ref[ne + 1 : 2 * ne + 1]
    return next_disp, node_terms * (1.0 / SPREAD)


def partial_product(first, second):
    grid = first[0] * second[0]
    total = jnp.sum(grid, axis=0, keepdims=True)
    nodes = jnp.sum(first[1] * second[1], axis=0, keepdims=True)
    lanes = grid.shape[1]
    for j in range(nodes.shape[1] // lanes):
        total = total + nodes[:, j * lanes : (j + 1) * lanes]
    return total


def places(sizes):
    return lax.axis_index("ea"), (lax.axis_index("gx") % 2 == 0, lax.axis_index("gy") % 2 == 0)


def ends():
    return [
        (lax.axis_index(axis) == 0, lax.axis_index(axis) == lax.axis_size(axis) - 1)
        for axis in ("gx", "gy")
    ]


def split_outs(sizes, refs):
    n_x, n_y, n_e = sizes["x_swaps"], sizes["y_swaps"], sizes["others"]
    return {"gx": refs[:n_x], "gy": refs[n_x : n_x + n_y], "ea": refs[n_x + n_y : n_x + n_y + n_e]}


def first_kernel(sizes, *refs):
    disp_ref, enr_ref, kind_ref, cell_ref, node_ref, coupling_ref = refs[:6]
    n = sizes["messages"]
    outs = split_outs(sizes, refs[6 : 6 + n])
    own_ref, disp_copy, enr_copy = refs[6 + n : 9 + n]
    hots = Hots(refs[9 + n : 13 + n])
    part_ref = refs[13 + n]
    me_ea, parity = places(sizes)
    hots.fill(sizes, kind_ref, cell_ref, node_ref, coupling_ref)
    disp = disp_ref[...].reshape(sizes["components"] * sizes["rows"], sizes["depth_z"])
    enriched = enr_ref[...]
    pack(sizes, hots, me_ea, parity, disp, enriched, outs, part_ref)
    own_ref[...] = part_ref[me_ea]
    disp_copy[...] = disp_ref[...]
    enr_copy[...] = enriched


def local_kernel(sizes, first, *refs):
    disp_ref, enr_ref = refs[:2]
    rows, dz = sizes["rows"], sizes["depth_z"]
    ne = sizes["enriched"]
    if first:
        shift_ref, diag_ref, off_ref, own_ref = refs[2:6]
        local_disp, local_enr, moment_ref, scale_ref, stiff_ref = refs[6:]
        scale_ref[...] = (6.0 - CENTRE) + shift_ref[...].reshape(rows, dz)
        diag = diag_ref[...] - CENTRE
        row = iota(diag.shape, 0)
        for q in range(ne):
            turned = jnp.concatenate([off_ref[p, q : q + 1] for p in range(ne)], axis=0)
            stiff_ref[q] = jnp.where(row == q, diag, 0.5 * (off_ref[q] + turned))
    else:
        own_ref, scale_ref, stiff_ref, local_disp, local_enr, moment_ref = refs[2:]
    disp = disp_ref[...].reshape(sizes["components"] * rows, dz)
    enriched = enr_ref[...]
    pushed = apply_local(sizes, disp, enriched, own_ref[...], scale_ref[...], stiff_ref)
    local_disp[...], local_enr[...] = pushed
    here = (disp, enriched)
    moment_ref[...] = partial_product(here, here)


def combine_kernel(sizes, last, *refs):
    n = sizes["messages"]
    local_disp, local_enr, disp_ref, enr_ref = refs[:4]
    hots = Hots(refs[4:8])
    got = split_outs(sizes, refs[8 : 8 + n])
    rest = refs[8 + n :]
    me_ea, parity = places(sizes)
    rows, dz, comps = sizes["rows"], sizes["depth_z"], sizes["components"]
    disp = disp_ref[...].reshape(comps * rows, dz)
    enriched = enr_ref[...]
    if last:
        moment_refs = rest[: 2 * ITERS - 1]
        next_disp_ref, next_enr_ref, sent_ref, held_ref = rest[2 * ITERS - 1 :]
    else:
        outs = split_outs(sizes, rest[:n])
        next_disp_ref, next_enr_ref, next_own_ref, moment_ref, part_ref, held_ref = rest[n:]
    local = (local_disp[...], local_enr[...])
    following = combine(sizes, hots, me_ea, parity, local, enriched, got, held_ref)
    next_disp_ref[...] = following[0].reshape(next_disp_ref.shape)
    next_enr_ref[...] = following[1]
    product = partial_product((disp, enriched), following)
    if last:
        row = iota((8, dz), 0)
        table = jnp.where(row == 2 * ITERS - 1, product, 0.0)
        for j, ref in enumerate(moment_refs):
            table = jnp.where(row == j, ref[...], table)
        sums = jnp.sum(table, axis=1, keepdims=True)
        spread = jnp.where(iota((8, dz), 1) == row, sums, 0.0)
        sent_ref[...] = jnp.broadcast_to(jnp.sum(spread, axis=0, keepdims=True)[None], sent_ref.shape)
    else:
        pack(sizes, hots, me_ea, parity, following[0], following[1], outs, part_ref)
        next_own_ref[...] = part_ref[me_ea]
        moment_ref[...] = product


def coefficients(moments):
    def product(first, second):
        total = 0.0
        for i, a in enumerate(first):
            for j, b in enumerate(second):
                total = total + a * b * moments[i + j]
        return total

    def image(vector):
        out = [CENTRE * a for a in vector] + [0.0]
        return [a + (SPREAD * vector[i - 1] if i else 0.0) for i, a in enumerate(out)]

    def combine(first, factor, second):
        length = max(len(first), len(second))
        out = []
        for i in range(length):
            a = first[i] if i < len(first) else None
            b = factor * second[i] if i < len(second) else None
            out.append(b if a is None else a if b is None else a + b)
        return out

    one = jnp.ones_like(moments[0])
    solution, residual, direction = [], [one], [one]
    norm_now = moments[0]
    for iteration in range(ITERS):
        along = image(direction)
        alpha = norm_now / product(direction, along)
        solution = combine(solution, alpha, direction)
        residual = combine(residual, -alpha, along)
        if iteration + 1 < ITERS:
            norm_next = product(residual, residual)
            direction = combine(residual, norm_next / norm_now, direction)
            norm_now = norm_next
    return solution, residual


def final_kernel(sizes, *refs):
    sums_ref = refs[0]
    disps, enrs = refs[1 : 2 + ITERS], refs[2 + ITERS : 3 + 2 * ITERS]
    x_disp, r_disp, x_enr, r_enr = refs[3 + 2 * ITERS :]
    row = jnp.sum(sums_ref[...], axis=0)
    lanes = row.shape[1]
    moments = jnp.sum(jnp.where(iota((8, lanes), 0) == iota((8, lanes), 1), row, 0.0), axis=1, keepdims=True)
    solution, residual = coefficients([moments[j : j + 1] for j in range(2 * ITERS)])

    def mix(factors, vectors, shape):
        total = None
        for factor, ref in zip(factors, vectors):
            value = ref[...]
            term = jnp.broadcast_to(factor.reshape((1,) * value.ndim), value.shape) * value
            total = term if total is None else total + term
        return total

    x_disp[...] = mix(solution, disps, None)
    r_disp[...] = mix(residual, disps, None)
    x_enr[...] = mix(solution, enrs, None)
    r_enr[...] = mix(residual, enrs, None)


def struct(*shape, dtype=F32):
    return pltpu.VMEM(shape, dtype)


def call(kernel, out_shape, name, scratch=(), flops=0):
    cost = pl.CostEstimate(flops=flops, bytes_accessed=0, transcendentals=0)
    run = pl.pallas_call(
        kernel, out_shape=out_shape, scratch_shapes=list(scratch), name=name, cost_estimate=cost
    )

    def with_args(given, kept):
        return run(*given, *(pltpu.with_memory_space_constraint(a, pltpu.VMEM) for a in kept))

    return with_args


def body(
    load_displacement,
    load_enriched,
    stiffness_shift,
    enriched_diag,
    enriched_off,
    coupling,
    slot_kind,
    slot_cell,
    slot_node,
):
    comps, dx, dy, dz = load_displacement.shape
    ne, nodes = load_enriched.shape
    owners = slot_kind.shape[1]
    counts = {axis: lax.axis_size(axis) for axis in AXES}
    perms_x = [p for p in (swap_pairs(counts, "gx", 0), swap_pairs(counts, "gx", 1)) if p]
    perms_y = [p for p in (swap_pairs(counts, "gy", 0), swap_pairs(counts, "gy", 1)) if p]
    perms_e = [partner_pairs(k, owners) for k in range(1, owners)]
    sizes = {
        "components": comps,
        "depth_x": dx,
        "depth_y": dy,
        "depth_z": dz,
        "rows": dx * dy,
        "enriched": ne,
        "nodes": nodes,
        "owners": owners,
        "capacity": slot_kind.shape[2],
        "x_swaps": len(perms_x),
        "y_swaps": len(perms_y),
        "others": len(perms_e),
        "messages": len(perms_x) + len(perms_y) + len(perms_e),
    }
    devices = counts["gx"] * counts["gy"] * counts["ea"]
    wide = max(nodes, comps * dx * dy)
    message_shapes = (
        [struct(comps, dy, dz)] * len(perms_x)
        + [struct(comps * dx, dz)] * len(perms_y)
        + [struct(2 * ne + 2, wide)] * len(perms_e)
    )
    routes = [(AXES, p) for p in perms_x + perms_y] + [("ea", p) for p in perms_e]
    part_scratch = pltpu.VMEM((owners, ne, nodes), F32)
    held_scratch = pltpu.VMEM((owners, 2 * ne + 2, wide), F32)
    vector = [struct(comps, dx, dy, dz), struct(ne, nodes)]
    flat_vector = [struct(comps * dx * dy, dz), struct(ne, nodes)]
    moment = struct(1, dz)
    n = sizes["messages"]

    outs = call(
        functools.partial(first_kernel, sizes),
        message_shapes + [struct(ne, nodes)] + vector + Hots.shapes(sizes),
        "first",
        [part_scratch],
    )((load_displacement, load_enriched, slot_kind, slot_cell, slot_node, coupling), ())
    messages, own, disps, enrs, hots = outs[:n], outs[n], [outs[n + 1]], [outs[n + 2]], outs[n + 3 :]
    moments, fixed = [], None
    for iteration in range(ITERS):
        received = [lax.ppermute(m, axis, pairs) for m, (axis, pairs) in zip(messages, routes)]
        here = (disps[-1], enrs[-1], own)
        first, last = iteration == 0, iteration + 1 == ITERS
        shapes = flat_vector + [moment]
        if first:
            shapes = shapes + [struct(dx * dy, dz), struct(ne, ne, nodes)]
        run = call(functools.partial(local_kernel, sizes, first), shapes, "local", flops=LOCAL_FLOPS)
        if first:
            given = (load_displacement, load_enriched)
            outs = run((*given, stiffness_shift, enriched_diag, enriched_off), (own,))
            fixed = outs[3:]
        else:
            outs = run((), (*here, *fixed))
        local = outs[:2]
        moments.append(outs[2])
        kept = (*local, *here[:2], *hots, *received)
        if last:
            disp, enr, sent = call(
                functools.partial(combine_kernel, sizes, True),
                vector + [struct(devices, 1, dz)],
                "last",
                [held_scratch],
            )((), (*kept, *moments))
        else:
            outs = call(
                functools.partial(combine_kernel, sizes, False),
                message_shapes + vector + [struct(ne, nodes), moment],
                "combine",
                [part_scratch, held_scratch],
            )((), kept)
            messages = outs[:n]
            disp, enr, own, product = outs[n:]
            moments.append(product)
        disps.append(disp)
        enrs.append(enr)
    sums = lax.all_to_all(sent, AXES, 0, 0, tiled=True)
    outs = [jax.ShapeDtypeStruct(a.shape, F32) for a in (disps[0], disps[0], enrs[0], enrs[0])]
    return call(functools.partial(final_kernel, sizes), outs, "final")((), (sums, *disps, *enrs))


def solution(mesh):
    placed = (
        P(None, "gx", "gy", "ea"),
        P(None, ("gx", "gy", "ea")),
        P("gx", "gy", "ea"),
        P(None, ("gx", "gy", "ea")),
        P(None, None, ("gx", "gy", "ea")),
        P(None, None, ("gx", "gy", "ea")),
        P(("gx", "gy", "ea"), None, None),
        P(("gx", "gy", "ea"), None, None),
        P(("gx", "gy", "ea"), None, None),
    )
    return jax.shard_map(
        body,
        mesh=mesh,
        in_specs=placed,
        out_specs=(
            P(None, "gx", "gy", "ea"),
            P(None, "gx", "gy", "ea"),
            P(None, ("gx", "gy", "ea")),
            P(None, ("gx", "gy", "ea")),
        ),
        check_vma=False,
    )
```

```python
import functools
import itertools
import math

import jax
import jax.numpy as jnp
from jax import lax
from jax.experimental import pallas as pl
from jax.experimental.pallas import tpu as pltpu
from jax.sharding import PartitionSpec as P

ITERS = 3
CENTRE = 11.0
SPREAD = 8.0
AXES = ("gx", "gy", "ea")
LOCAL_FLOPS = 2000000
F32 = jnp.float32
BF16 = jnp.bfloat16


def swap_pairs(counts, axis, first):
    count, at = counts[axis], AXES.index(axis)
    if first + 1 >= count:
        return []
    sizes = [counts[a] for a in AXES]
    pairs = []
    for place in itertools.product(*(range(n) for n in sizes)):
        other = list(place)
        mate = first + ((place[at] - first) ^ 1)
        if place[at] >= first and mate < count:
            other[at] = mate
        elif sizes[-1] % 2 == 0:
            other[-1] = place[-1] ^ 1
        flat = [sum(p * math.prod(sizes[j + 1 :]) for j, p in enumerate(x)) for x in (place, other)]
        pairs.append(tuple(flat))
    return pairs


def partner(me, step, count):
    return me ^ step if count & (count - 1) == 0 else lax.rem(me + step, count)


def slot_of(me, owner, count):
    return me ^ owner if count & (count - 1) == 0 else lax.rem(me - owner + count, count)


def partner_pairs(step, count):
    if count & (count - 1) == 0:
        return [(i, i ^ step) for i in range(count)]
    return [(i, (i + step) % count) for i in range(count)]


def halves(value):
    high = value.astype(BF16)
    low = (value - high.astype(F32)).astype(BF16)
    return high, low


def iota(shape, dim):
    return lax.broadcasted_iota(jnp.int32, shape, dim)


def one_hot(flag):
    return jnp.where(flag, 1.0, 0.0).astype(BF16)


def dot(left, right, dims):
    return lax.dot_general(left, right, (dims, ((), ())), preferred_element_type=F32)


NN = ((1,), (0,))
NT = ((1,), (1,))
TN = ((0,), (0,))


class Hots:
    def __init__(self, refs):
        self.weights, self.row_hot, self.z_hot, self.node_hot = refs

    @staticmethod
    def shapes(sizes):
        total = sizes["owners"] * sizes["capacity"]
        return [
            struct(sizes["components"], sizes["enriched"], total),
            struct(sizes["rows"], total),
            struct(sizes["depth_z"], total, dtype=BF16),
            struct(sizes["owners"], sizes["nodes"], sizes["capacity"], dtype=BF16),
        ]

    def fill(self, sizes, kind_ref, cell_ref, node_ref, coupling_ref):
        owners, capacity = sizes["owners"], sizes["capacity"]
        total = owners * capacity
        rows, depth_z = sizes["rows"], sizes["depth_z"]
        cells = jnp.concatenate([cell_ref[0, o : o + 1, :] for o in range(owners)], axis=1)
        kinds = jnp.concatenate([kind_ref[0, o : o + 1, :] for o in range(owners)], axis=1)
        cell_row = cells // depth_z
        cell_z = cells - cell_row * depth_z
        self.row_hot[...] = jnp.where(iota((rows, total), 0) == cell_row, 1.0, 0.0)
        self.z_hot[...] = one_hot(iota((depth_z, total), 0) == cell_z)
        for o in range(owners):
            self.node_hot[o] = one_hot(
                iota((sizes["nodes"], capacity), 0) == node_ref[0, o : o + 1, :]
            )
        heaviside = jnp.where(kinds >= 1, 1.0, 0.0)
        tip = jnp.where(kinds == 2, 1.0, 0.0)
        masks = jnp.where(iota((sizes["enriched"], total), 0) < 3, heaviside, tip)
        for p in range(sizes["components"]):
            self.weights[p] = coupling_ref[p] * masks


def message_shape(sizes):
    wide = max(sizes["nodes"], sizes["components"] * sizes["rows"])
    x_rows = -(-sizes["components"] // (wide // sizes["depth_z"])) * sizes["depth_y"]
    return max(2 * sizes["enriched"] + 2, x_rows, sizes["components"] * sizes["depth_x"]), wide


def x_place(sizes, component):
    dy, dz = sizes["depth_y"], sizes["depth_z"]
    row, column = divmod(component, message_shape(sizes)[1] // dz)
    return slice(row * dy, (row + 1) * dy), slice(column * dz, (column + 1) * dz)


def pack(sizes, hots, me_ea, parity, disp, enriched, outs, part_ref):
    comps, dx, dy, dz, rows, ne = (
        sizes[k] for k in ("components", "depth_x", "depth_y", "depth_z", "rows", "enriched")
    )
    owners, capacity = sizes["owners"], sizes["capacity"]
    grid = disp.reshape(comps, dx, dy, dz)
    even_x, even_y = parity
    for j, out in enumerate(outs["gx"]):
        for p in range(comps):
            rows_of, lanes_of = x_place(sizes, p)
            out[rows_of, lanes_of] = jnp.where(even_x == (j == 0), grid[p, dx - 1], grid[p, 0])
    lines = disp.reshape(comps * dx, dy, dz)
    for j, out in enumerate(outs["gy"]):
        out[: comps * dx, :dz] = jnp.where(even_y == (j == 0), lines[:, dy - 1], lines[:, 0])
    high, low = halves(disp)
    columns = dot(jnp.concatenate([high, low], axis=0), hots.z_hot[...], NN)
    columns = columns[: comps * rows] + columns[comps * rows :]
    to_nodes = None
    for p in range(comps):
        picked = jnp.sum(hots.row_hot[...] * columns[p * rows : (p + 1) * rows], axis=0, keepdims=True)
        term = hots.weights[p] * picked
        to_nodes = term if to_nodes is None else to_nodes + term
    node_high, node_low = halves(to_nodes)
    for o in range(owners):
        block = slice(o * capacity, (o + 1) * capacity)
        part_ref[o] = dot(node_high[:, block], hots.node_hot[o], NT) + dot(
            node_low[:, block], hots.node_hot[o], NT
        )
    edge = one_hot(
        (iota((8, dz), 0) == 0) & (iota((8, dz), 1) == 0)
        | (iota((8, dz), 0) == 1) & (iota((8, dz), 1) == dz - 1)
    )
    faces = dot(edge, high, NT) + dot(edge, low, NT)
    for k, out in enumerate(outs["ea"]):
        out[:ne, : sizes["nodes"]] = enriched
        out[ne + 1 : 2 * ne + 1, : sizes["nodes"]] = part_ref[partner(me_ea, k + 1, owners)]
        out[ne : ne + 1, : comps * rows] = faces[0:1]
        out[2 * ne + 1 : 2 * ne + 2, : comps * rows] = faces[1:2]


def slots_to_cells(sizes, hots, values):
    comps, rows = sizes["components"], sizes["rows"]
    spread_high, spread_low = [], []
    for p in range(comps):
        to_cells = jnp.sum(hots.weights[p] * values, axis=0, keepdims=True)
        c_high, c_low = halves(to_cells)
        spread_high.append((hots.row_hot[...] * c_high.astype(F32)).astype(BF16))
        spread_low.append((hots.row_hot[...] * c_low.astype(F32)).astype(BF16))
    added = dot(jnp.concatenate(spread_high + spread_low, axis=0), hots.z_hot[...], NT)
    return added[: comps * rows] + added[comps * rows :]


def apply_local(sizes, disp, enriched, own_part, scale, stiff_ref):
    comps, dx, dy, dz, rows, ne = (
        sizes[k] for k in ("components", "depth_x", "depth_y", "depth_z", "rows", "enriched")
    )
    grid = disp.reshape(comps, dx, dy, dz)
    no_x = jnp.zeros((comps, 1, dy, dz), F32)
    beside = jnp.concatenate([grid[:, 1:], no_x], axis=1) + jnp.concatenate([no_x, grid[:, :-1]], axis=1)
    beside = beside.reshape(comps * rows, dz)
    total_rows = comps * rows
    y_place = iota((total_rows, dz), 0) % dy
    beside = beside + jnp.where(y_place == 0, 0.0, pltpu.roll(disp, 1, 0))
    beside = beside + jnp.where(y_place == dy - 1, 0.0, pltpu.roll(disp, total_rows - 1, 0))
    z_place = iota((total_rows, dz), 1)
    beside = beside + jnp.where(z_place == 0, 0.0, pltpu.roll(disp, 1, 1))
    beside = beside + jnp.where(z_place == dz - 1, 0.0, pltpu.roll(disp, dz - 1, 1))
    scaled = (scale[None] * disp.reshape(comps, rows, dz)).reshape(total_rows, dz)
    pushed = own_part
    for q in range(ne):
        pushed = pushed + stiff_ref[q] * enriched[q : q + 1]
    return scaled - beside, pushed


def combine(sizes, hots, me_ea, parity, local, enriched, got, held_ref):
    comps, dx, dy, dz, rows, ne = (
        sizes[k] for k in ("components", "depth_x", "depth_y", "depth_z", "rows", "enriched")
    )
    owners = sizes["owners"]
    total_rows = comps * rows
    local_disp, local_enriched = local
    held_ref[0, :ne, : sizes["nodes"]] = enriched
    for k, ref in enumerate(got["ea"]):
        held_ref[k + 1] = ref[: 2 * ne + 2]
    values = []
    for o in range(owners):
        w_high, w_low = halves(held_ref[slot_of(me_ea, o, owners), :ne, : sizes["nodes"]])
        values.append(dot(w_high, hots.node_hot[o], NN) + dot(w_low, hots.node_hot[o], NN))
    added = slots_to_cells(sizes, hots, jnp.concatenate(values, axis=1))
    even_x, even_y = parity
    zero_x = jnp.zeros((comps, dy, dz), F32)
    zero_y = jnp.zeros((comps * dx, dz), F32)

    def x_face(ref):
        return jnp.stack([ref[x_place(sizes, p)] for p in range(comps)])

    x_a = x_face(got["gx"][0]) if len(got["gx"]) > 0 else zero_x
    x_b = x_face(got["gx"][1]) if len(got["gx"]) > 1 else zero_x
    y_a = got["gy"][0][: comps * dx, :dz] if len(got["gy"]) > 0 else zero_y
    y_b = got["gy"][1][: comps * dx, :dz] if len(got["gy"]) > 1 else zero_y
    (first_x, last_x), (first_y, last_y) = ends()
    below_x = jnp.where(first_x, 0.0, jnp.where(even_x, x_b, x_a))
    above_x = jnp.where(last_x, 0.0, jnp.where(even_x, x_a, x_b))
    below_y = jnp.where(first_y, 0.0, jnp.where(even_y, y_b, y_a))
    above_y = jnp.where(last_y, 0.0, jnp.where(even_y, y_a, y_b))
    no_x = jnp.zeros((comps, dx - 2, dy, dz), F32)
    beside = jnp.concatenate([below_x[:, None], no_x, above_x[:, None]], axis=1).reshape(total_rows, dz)
    y_place = iota((total_rows, dz), 0) % dy
    spread_y = (comps * dx, dy, dz)
    low_y = jnp.broadcast_to(below_y[:, None, :], spread_y).reshape(total_rows, dz)
    high_y = jnp.broadcast_to(above_y[:, None, :], spread_y).reshape(total_rows, dz)
    beside = beside + jnp.where(y_place == 0, low_y, jnp.where(y_place == dy - 1, high_y, 0.0))
    below = jnp.maximum(me_ea - 1, 0)
    above = jnp.minimum(me_ea + 1, owners - 1)
    low_z = held_ref[slot_of(me_ea, below, owners), 2 * ne + 1 : 2 * ne + 2, :total_rows]
    high_z = held_ref[slot_of(me_ea, above, owners), ne : ne + 1, :total_rows]
    low_z = jnp.where(me_ea > 0, low_z, 0.0)
    high_z = jnp.where(me_ea < owners - 1, high_z, 0.0)
    line = iota((8, total_rows), 0)
    lows, highs = halves(low_z), halves(high_z)
    sides = jnp.zeros((8, total_rows), F32)
    for j, part in enumerate((lows[0], lows[1], highs[0], highs[1])):
        sides = jnp.where(line == j, part.astype(F32), sides)
    edge_row, edge_lane = iota((8, dz), 0), iota((8, dz), 1)
    edge = one_hot(
        (edge_row < 2) & (edge_lane == 0) | (edge_row >= 2) & (edge_row < 4) & (edge_lane == dz - 1)
    )
    beside = beside + dot(sides.astype(BF16), edge, TN)
    next_disp = (local_disp - beside + added) * (1.0 / SPREAD)
    node_terms = local_enriched
    for ref in got["ea"]:
        node_terms = node_terms + ref[ne + 1 : 2 * ne + 1, : sizes["nodes"]]
    return next_disp, node_terms * (1.0 / SPREAD)


def partial_product(first, second):
    grid = first[0] * second[0]
    total = jnp.sum(grid, axis=0, keepdims=True)
    nodes = jnp.sum(first[1] * second[1], axis=0, keepdims=True)
    lanes = grid.shape[1]
    for j in range(nodes.shape[1] // lanes):
        total = total + nodes[:, j * lanes : (j + 1) * lanes]
    return total


def places(sizes):
    return lax.axis_index("ea"), (lax.axis_index("gx") % 2 == 0, lax.axis_index("gy") % 2 == 0)


def ends():
    return [
        (lax.axis_index(axis) == 0, lax.axis_index(axis) == lax.axis_size(axis) - 1)
        for axis in ("gx", "gy")
    ]


def split_outs(sizes, refs):
    out = {"gx": [], "gy": [], "ea": []}
    for (kind, _), ref in sorted(zip(sizes["order"], refs), key=lambda pair: pair[0]):
        out[kind].append(ref)
    return out


def first_kernel(sizes, *refs):
    disp_ref, enr_ref, kind_ref, cell_ref, node_ref, coupling_ref = refs[:6]
    n = sizes["messages"]
    outs = split_outs(sizes, refs[6 : 6 + n])
    own_ref, disp_copy, enr_copy = refs[6 + n : 9 + n]
    hots = Hots(refs[9 + n : 13 + n])
    part_ref = refs[13 + n]
    me_ea, parity = places(sizes)
    hots.fill(sizes, kind_ref, cell_ref, node_ref, coupling_ref)
    disp = disp_ref[...].reshape(sizes["components"] * sizes["rows"], sizes["depth_z"])
    enriched = enr_ref[...]
    pack(sizes, hots, me_ea, parity, disp, enriched, outs, part_ref)
    own_ref[...] = part_ref[me_ea]
    disp_copy[...] = disp_ref[...]
    enr_copy[...] = enriched


def local_kernel(sizes, first, *refs):
    disp_ref, enr_ref = refs[:2]
    rows, dz = sizes["rows"], sizes["depth_z"]
    ne = sizes["enriched"]
    if first:
        shift_ref, diag_ref, off_ref, own_ref = refs[2:6]
        local_disp, local_enr, moment_ref, scale_ref, stiff_ref = refs[6:]
        scale_ref[...] = (6.0 - CENTRE) + shift_ref[...].reshape(rows, dz)
        diag = diag_ref[...] - CENTRE
        row = iota(diag.shape, 0)
        for q in range(ne):
            turned = jnp.concatenate([off_ref[p, q : q + 1] for p in range(ne)], axis=0)
            stiff_ref[q] = jnp.where(row == q, diag, 0.5 * (off_ref[q] + turned))
    else:
        own_ref, scale_ref, stiff_ref, local_disp, local_enr, moment_ref = refs[2:]
    disp = disp_ref[...].reshape(sizes["components"] * rows, dz)
    enriched = enr_ref[...]
    pushed = apply_local(sizes, disp, enriched, own_ref[...], scale_ref[...], stiff_ref)
    local_disp[...], local_enr[...] = pushed
    here = (disp, enriched)
    moment_ref[...] = partial_product(here, here)


def combine_kernel(sizes, last, *refs):
    n = sizes["messages"]
    local_disp, local_enr, disp_ref, enr_ref = refs[:4]
    hots = Hots(refs[4:8])
    got = split_outs(sizes, refs[8 : 8 + n])
    rest = refs[8 + n :]
    me_ea, parity = places(sizes)
    rows, dz, comps = sizes["rows"], sizes["depth_z"], sizes["components"]
    disp = disp_ref[...].reshape(comps * rows, dz)
    enriched = enr_ref[...]
    if last:
        moment_refs = rest[: 2 * ITERS - 1]
        next_disp_ref, next_enr_ref, sent_ref, held_ref = rest[2 * ITERS - 1 :]
    else:
        outs = split_outs(sizes, rest[:n])
        next_disp_ref, next_enr_ref, next_own_ref, moment_ref, part_ref, held_ref = rest[n:]
    local = (local_disp[...], local_enr[...])
    following = combine(sizes, hots, me_ea, parity, local, enriched, got, held_ref)
    next_disp_ref[...] = following[0].reshape(next_disp_ref.shape)
    next_enr_ref[...] = following[1]
    product = partial_product((disp, enriched), following)
    if last:
        row = iota((8, dz), 0)
        table = jnp.where(row == 2 * ITERS - 1, product, 0.0)
        for j, ref in enumerate(moment_refs):
            table = jnp.where(row == j, ref[...], table)
        sums = jnp.sum(table, axis=1, keepdims=True)
        spread = jnp.where(iota((8, dz), 1) == row, sums, 0.0)
        sent_ref[...] = jnp.broadcast_to(jnp.sum(spread, axis=0, keepdims=True)[None], sent_ref.shape)
    else:
        pack(sizes, hots, me_ea, parity, following[0], following[1], outs, part_ref)
        next_own_ref[...] = part_ref[me_ea]
        moment_ref[...] = product


def coefficients(moments):
    def product(first, second):
        total = 0.0
        for i, a in enumerate(first):
            for j, b in enumerate(second):
                total = total + a * b * moments[i + j]
        return total

    def image(vector):
        out = [CENTRE * a for a in vector] + [0.0]
        return [a + (SPREAD * vector[i - 1] if i else 0.0) for i, a in enumerate(out)]

    def combine(first, factor, second):
        length = max(len(first), len(second))
        out = []
        for i in range(length):
            a = first[i] if i < len(first) else None
            b = factor * second[i] if i < len(second) else None
            out.append(b if a is None else a if b is None else a + b)
        return out

    one = jnp.ones_like(moments[0])
    solution, residual, direction = [], [one], [one]
    norm_now = moments[0]
    for iteration in range(ITERS):
        along = image(direction)
        alpha = norm_now / product(direction, along)
        solution = combine(solution, alpha, direction)
        residual = combine(residual, -alpha, along)
        if iteration + 1 < ITERS:
            norm_next = product(residual, residual)
            direction = combine(residual, norm_next / norm_now, direction)
            norm_now = norm_next
    return solution, residual


def final_kernel(sizes, *refs):
    sums_ref = refs[0]
    disps, enrs = refs[1 : 2 + ITERS], refs[2 + ITERS : 3 + 2 * ITERS]
    x_disp, r_disp, x_enr, r_enr = refs[3 + 2 * ITERS :]
    row = jnp.sum(sums_ref[...], axis=0)
    lanes = row.shape[1]
    moments = jnp.sum(jnp.where(iota((8, lanes), 0) == iota((8, lanes), 1), row, 0.0), axis=1, keepdims=True)
    solution, residual = coefficients([moments[j : j + 1] for j in range(2 * ITERS)])

    def mix(factors, vectors, shape):
        total = None
        for factor, ref in zip(factors, vectors):
            value = ref[...]
            term = jnp.broadcast_to(factor.reshape((1,) * value.ndim), value.shape) * value
            total = term if total is None else total + term
        return total

    x_disp[...] = mix(solution, disps, None)
    r_disp[...] = mix(residual, disps, None)
    x_enr[...] = mix(solution, enrs, None)
    r_enr[...] = mix(residual, enrs, None)


def struct(*shape, dtype=F32):
    return pltpu.VMEM(shape, dtype)


def call(kernel, out_shape, name, scratch=(), flops=0):
    cost = pl.CostEstimate(flops=flops, bytes_accessed=0, transcendentals=0)
    run = pl.pallas_call(
        kernel, out_shape=out_shape, scratch_shapes=list(scratch), name=name, cost_estimate=cost
    )

    def with_args(given, kept):
        return run(*given, *(pltpu.with_memory_space_constraint(a, pltpu.VMEM) for a in kept))

    return with_args


def body(
    load_displacement,
    load_enriched,
    stiffness_shift,
    enriched_diag,
    enriched_off,
    coupling,
    slot_kind,
    slot_cell,
    slot_node,
):
    comps, dx, dy, dz = load_displacement.shape
    ne, nodes = load_enriched.shape
    owners = slot_kind.shape[1]
    counts = {axis: lax.axis_size(axis) for axis in AXES}
    perms_x = [p for p in (swap_pairs(counts, "gx", 0), swap_pairs(counts, "gx", 1)) if p]
    perms_y = [p for p in (swap_pairs(counts, "gy", 0), swap_pairs(counts, "gy", 1)) if p]
    perms_e = [partner_pairs(k, owners) for k in range(1, owners)]
    kinds = {"gx": perms_x, "gy": perms_y, "ea": perms_e}
    order = [("gy", j) for j in range(len(perms_y))]
    order += [("ea", j) for j in reversed(range(1, len(perms_e)))]
    order += [("gx", j) for j in range(len(perms_x))]
    order += [("ea", 0)] if perms_e else []
    sizes = {
        "components": comps,
        "depth_x": dx,
        "depth_y": dy,
        "depth_z": dz,
        "rows": dx * dy,
        "enriched": ne,
        "nodes": nodes,
        "owners": owners,
        "capacity": slot_kind.shape[2],
        "order": order,
        "messages": len(order),
    }
    devices = counts["gx"] * counts["gy"] * counts["ea"]
    message_shapes = [struct(*message_shape(sizes))] * len(order)
    routes = [("ea" if kind == "ea" else AXES, kinds[kind][j]) for kind, j in order]
    part_scratch = pltpu.VMEM((owners, ne, nodes), F32)
    held_scratch = pltpu.VMEM((owners, 2 * ne + 2, message_shape(sizes)[1]), F32)
    vector = [struct(comps, dx, dy, dz), struct(ne, nodes)]
    flat_vector = [struct(comps * dx * dy, dz), struct(ne, nodes)]
    moment = struct(1, dz)
    n = sizes["messages"]

    outs = call(
        functools.partial(first_kernel, sizes),
        message_shapes + [struct(ne, nodes)] + vector + Hots.shapes(sizes),
        "first",
        [part_scratch],
    )((load_displacement, load_enriched, slot_kind, slot_cell, slot_node, coupling), ())
    messages, own, disps, enrs, hots = outs[:n], outs[n], [outs[n + 1]], [outs[n + 2]], outs[n + 3 :]
    moments, fixed = [], None
    for iteration in range(ITERS):
        received = [lax.ppermute(m, axis, pairs) for m, (axis, pairs) in zip(messages, routes)]
        here = (disps[-1], enrs[-1], own)
        first, last = iteration == 0, iteration + 1 == ITERS
        shapes = flat_vector + [moment]
        if first:
            shapes = shapes + [struct(dx * dy, dz), struct(ne, ne, nodes)]
        run = call(functools.partial(local_kernel, sizes, first), shapes, "local", flops=LOCAL_FLOPS)
        if first:
            given = (load_displacement, load_enriched)
            outs = run((*given, stiffness_shift, enriched_diag, enriched_off), (own,))
            fixed = outs[3:]
        else:
            outs = run((), (*here, *fixed))
        local = outs[:2]
        moments.append(outs[2])
        kept = (*local, *here[:2], *hots, *received)
        if last:
            disp, enr, sent = call(
                functools.partial(combine_kernel, sizes, True),
                vector + [struct(devices, 1, dz)],
                "last",
                [held_scratch],
            )((), (*kept, *moments))
        else:
            outs = call(
                functools.partial(combine_kernel, sizes, False),
                message_shapes + vector + [struct(ne, nodes), moment],
                "combine",
                [part_scratch, held_scratch],
            )((), kept)
            messages = outs[:n]
            disp, enr, own, product = outs[n:]
            moments.append(product)
        disps.append(disp)
        enrs.append(enr)
    sums = lax.all_to_all(sent, AXES, 0, 0, tiled=True)
    outs = [jax.ShapeDtypeStruct(a.shape, F32) for a in (disps[0], disps[0], enrs[0], enrs[0])]
    return call(functools.partial(final_kernel, sizes), outs, "final")((), (sums, *disps, *enrs))


def solution(mesh):
    placed = (
        P(None, "gx", "gy", "ea"),
        P(None, ("gx", "gy", "ea")),
        P("gx", "gy", "ea"),
        P(None, ("gx", "gy", "ea")),
        P(None, None, ("gx", "gy", "ea")),
        P(None, None, ("gx", "gy", "ea")),
        P(("gx", "gy", "ea"), None, None),
        P(("gx", "gy", "ea"), None, None),
        P(("gx", "gy", "ea"), None, None),
    )
    return jax.shard_map(
        body,
        mesh=mesh,
        in_specs=placed,
        out_specs=(
            P(None, "gx", "gy", "ea"),
            P(None, "gx", "gy", "ea"),
            P(None, ("gx", "gy", "ea")),
            P(None, ("gx", "gy", "ea")),
        ),
        check_vma=False,
    )
```
